128 devices in a mesh: brick: 32 (over z, y, core), mode: 4 (over x).
Axes of the slice: x: 4, y: 4, z: 4, core: 2. Of those that a mesh axis runs over, the one named last changes fastest.
Arguments:
- coeffs: float32 [32768, 3072], P('brick', 'mode'), may hold values from -6 to 6
- weights: bfloat16 [2, 1536, 32, 1024], P(None, 'brick'), may hold values from -0.1875 to 0.1875
- owners: int32 [2, 1536, 1], P(None, 'brick'), may hold values from 0 to 31; in each aligned block of 48 rows (0 to 47, 48 to 95, ..., all dimensions but the last counted through in order) at most 2 rows name the same one
- offsets: int32 [2, 1536], P(None, 'brick'), may hold values from 0 to 7
- mode_basis: bfloat16 [2, 3072, 1024], P(None, 'mode'), may hold values from -0.109375 to 0.109375
- measured: float32 [2, 8192, 1024], P(None, ('brick', 'mode')), may hold values from -6 to 6
Outputs:
- coeffs_out: float32 [32768, 3072], P('brick', 'mode')
- residual: float32 [2, 8192, 1024], P(None, ('brick', 'mode'))
The draws below stay inside these ranges and needn't reach their ends.
Inputs may be any that keep to these rules, and one draw needn't show every extreme that they name: `owners`: among the 48 entries of one brick in one view, no owner is named more than 2 times.
All inputs are finite; a program needn't handle non-finite values.
Results may differ from the reference program's by a relative error of at most 0.0098.
Values may be sent and summed in bfloat16 or wider, within the bound.
A program may use at most 128 MiB of HBM per device.

```python
import math
import jax
import jax.numpy as jnp
import numpy as np
from jax import lax

M = 3072
BINS = 1024
VOX_DEV = 1024
RB = 32
BLK_DEV = 8
SLOTS = 48
VIEWS = 2
ITERS = 2
CAP = 2
RAYS = 8192
VOX = 32768
N_BRICK = 32


def touch_ends(entries, rng, smallest, top_value):
    dims = entries.shape
    place = [jax.random.randint(jax.random.fold_in(rng, axis), (), 0, dims[axis]) for axis in range(len(dims))]
    entries = entries.at[tuple(place)].set(smallest)
    longest = dims.index(max(dims))
    place[longest] = (place[longest] + 1) % dims[longest]
    return entries.at[tuple(place)].set(top_value)


def levels(stream_key, shape, shards, least, top_value):
    gain = 1.0
    for position, parts in shards:
        draws = jax.random.uniform(jax.random.fold_in(jax.random.fold_in(stream_key, 6), position), (parts,), jnp.float32, least / len(shards), top_value / len(shards))
        gain = gain * jnp.repeat(jnp.exp(draws), shape[position] // parts).reshape((-1,) + (1,) * (len(shape) - 1 - position))
    return gain


def shared_out(own_key, own, number, rows, amount, top, bound, lean):
    order = jax.random.permutation(own_key, amount)
    packed, ordinary = shares(amount, rows * top, bound, lean, True), shares(amount, rows * top, bound, lean, False)
    places = jnp.arange(amount)

    def named(tallies, turn):
        used = int((tallies > 0).sum())
        fixed = max(1, used // 4)
        passed = fixed + (places - fixed + turn * (used - fixed)) % max(1, amount - fixed)
        return jnp.zeros((amount,), jnp.int32).at[order[jnp.where(places < fixed, places, passed)]].set(jnp.asarray(tallies, jnp.int32))

    tallies = jnp.where(number % 4 == 0, named(packed, number // 4), named(ordinary, number - number // 4 - 1))
    mixed = jax.random.permutation(jax.random.fold_in(own, 3), amount)
    giver, taker = mixed[0:amount // 2 * 2:2], mixed[1:amount // 2 * 2:2]
    slack = jnp.minimum(tallies[giver] - 1, bound - tallies[taker]) // 2
    slack = jnp.where((giver == order[0]) | (taker == order[0]) | (tallies[taker] == 0), 0, jnp.maximum(slack, 0))
    passed = jax.random.randint(jax.random.fold_in(own, 4), (amount // 2,), 0, 1 << 20) % (slack + 1)
    tallies = tallies.at[giver].add(-passed).at[taker].add(passed)
    members = jnp.searchsorted(jnp.cumsum(tallies), jnp.arange(rows * top), side="right").astype(jnp.int32)
    table = members.reshape(top, rows).T
    table = table[jax.random.permutation(jax.random.fold_in(own, 1), rows)]
    turn = jax.random.randint(jax.random.fold_in(own, 2), (rows, 1), 0, top)
    return jnp.take_along_axis(table, (jnp.arange(top)[None, :] + turn) % top, axis=1)


def shares(amount, total, reach, slope, full):
    weights = [(1 << 20) // math.isqrt(standing ** slope) + 1 for standing in range(1, amount + 1)]
    largest = reach if full else min(reach, max(-(-total // amount), total * weights[0] // sum(weights)))
    least = 1 if total - largest >= amount - 1 else 0
    given, rest = [largest] + [least] * (amount - 1), total - largest - least * (amount - 1)
    while rest > 0:
        movable = [i for i in range(1, amount) if given[i] < largest] or [i for i in range(1, amount) if given[i] < reach]
        pool, remaining = sum([weights[i] for i in movable]), rest
        for i in movable:
            more = min(reach - given[i], max(1, remaining * weights[i] // pool), rest)
            given[i] = given[i] + more
            rest = rest - more
    return np.array(given)


def normal_values(key, extent, scale, limit, pieces=(), kind=jnp.bfloat16):
    entries = scale * jax.random.normal(key, extent, jnp.float32)
    if pieces:
        entries = entries * levels(key, extent, pieces, -0.22, 0.18)
    return jnp.clip(entries, -limit, limit).astype(kind)


def setup_inputs(seed: int = 0) -> dict:
    key_of = jax.random.split(jax.random.key(seed), 7)
    coeffs = normal_values(key_of[0], (VOX, M), 1.0, 6.0, ((0, 32), (1, 4)), jnp.float32)
    weights = normal_values(key_of[1], (VIEWS, N_BRICK * SLOTS, RB, VOX_DEV), VOX_DEV ** -0.5, 0.1875, ((1, 32),))
    owners_keys = jax.random.split(jax.random.fold_in(key_of[2], 1), VIEWS * (N_BRICK * SLOTS) // SLOTS)
    owners_turns = jax.random.permutation(jax.random.fold_in(key_of[2], 3), VIEWS * (N_BRICK * SLOTS) // SLOTS)
    owners = jax.vmap(lambda own, number: shared_out(jax.random.fold_in(key_of[2], 2), own, number, SLOTS, N_BRICK, 1, CAP, 2))(owners_keys, owners_turns).reshape((VIEWS, N_BRICK * SLOTS, 1))
    offsets = touch_ends(jax.random.randint(key_of[3], (VIEWS, N_BRICK * SLOTS), 0, BLK_DEV), jax.random.fold_in(key_of[3], 1), 0, BLK_DEV - 1).astype(jnp.int32)
    mode_basis = normal_values(key_of[4], (VIEWS, M, BINS), M ** -0.5, 0.109375, ((1, 4),))
    measured = normal_values(key_of[5], (VIEWS, RAYS, BINS), 1.0, 6.0, ((1, 128),), jnp.float32)
    return {"coeffs": coeffs, "weights": weights, "owners": owners, "offsets": offsets, "mode_basis": mode_basis, "measured": measured}


LEARN_RATE = 0.2


def brick_forward(pair_args):
    return jnp.dot(pair_args[0], pair_args[1], preferred_element_type=jnp.float32).astype(jnp.bfloat16)


def brick_adjoint(pair_args):
    return lax.dot_general(pair_args[0], pair_args[1], (((0,), (0,)), ((), ())), preferred_element_type=jnp.float32)


def reference(coeffs, weights, owners, offsets, mode_basis, measured):
    vox_total, mode_total = coeffs.shape
    block_ids = (owners[:, :, 0] * BLK_DEV + offsets).astype(jnp.int32)
    residuals = []
    for step_index in range(ITERS):
        low_coeffs = coeffs.astype(jnp.bfloat16).reshape(N_BRICK, VOX_DEV, mode_total)
        update = jnp.zeros((N_BRICK, VOX_DEV, mode_total), jnp.float32)
        residuals = []
        for view_index in range(VIEWS):
            brick_weights = weights[view_index].reshape(N_BRICK, SLOTS * RB, VOX_DEV)
            slot_proj = lax.map(brick_forward, (brick_weights, low_coeffs))
            slot_proj = slot_proj.reshape(N_BRICK * SLOTS, RB, mode_total)
            summed = jnp.zeros((N_BRICK * BLK_DEV, RB, mode_total), jnp.float32)
            summed = summed.at[block_ids[view_index]].add(slot_proj.astype(jnp.float32))
            low_rays = summed.reshape(RAYS, mode_total).astype(jnp.bfloat16)
            intensity = jnp.dot(low_rays, mode_basis[view_index], preferred_element_type=jnp.float32)
            residual = intensity - measured[view_index]
            residuals.append(residual)
            grad_rays = jnp.dot(residual.astype(jnp.bfloat16), mode_basis[view_index].T,
                                preferred_element_type=jnp.float32).astype(jnp.bfloat16)
            grad_blocks = grad_rays.reshape(N_BRICK * BLK_DEV, RB, mode_total)
            picked = grad_blocks[block_ids[view_index]].reshape(N_BRICK, SLOTS * RB, mode_total)
            update = update + lax.map(brick_adjoint, (brick_weights, picked))
        coeffs = coeffs - LEARN_RATE * update.reshape(vox_total, mode_total)
    return coeffs, jnp.stack(residuals)
```

```python
import jax
import jax.numpy as jnp
from jax import lax
from jax.sharding import PartitionSpec as P

BLK_DEV = 8
LEARN_RATE = 0.2
BF = jnp.bfloat16
F32 = jnp.float32


def dot(a, b, dims=((1,), (0,))):
    return lax.dot_general(a, b, (dims, ((), ())), preferred_element_type=F32)


def slot_tables(owner_list, offset_list, peer_count, capacity):
    slots = owner_list.shape[0]
    order = jnp.arange(slots, dtype=jnp.int32)
    same = owner_list[:, None] == owner_list[None, :]
    earlier = jnp.sum((same & (order[None, :] < order[:, None])).astype(jnp.int32), 1)
    places = owner_list * capacity + earlier
    hits = places[None, :] == jnp.arange(peer_count * capacity, dtype=jnp.int32)[:, None]
    hits = hits.astype(jnp.int32)
    source = jnp.sum(hits * order[None, :], 1)
    used = jnp.sum(hits, 1)
    labels = jnp.sum(hits * (offset_list[None, :] + 1), 1) - 1
    return source, used, labels


def swap(x, axis):
    return lax.all_to_all(x, axis, split_axis=0, concat_axis=0, tiled=True)


def bins_to_front(x, parts):
    rows, bins = x.shape
    return jnp.moveaxis(x.reshape(rows, parts, bins // parts), 1, 0)


def shards(coeffs, weights, owners, offsets, basis, measured):
    peers, modes = lax.axis_size("brick"), lax.axis_size("mode")
    views, slots, ray_block, voxels = weights.shape
    capacity = max(2, slots // peers + 1)
    bins = basis.shape[2]
    mine = bins // modes
    places = peers * capacity
    rays = BLK_DEV * ray_block
    brick = lax.axis_index("brick")

    tables = [
        slot_tables(owners[v, :, 0], offsets[v], peers, capacity) for v in range(views)
    ]
    labels = jnp.stack([t[2] for t in tables], 0).reshape(views, peers, capacity)
    labels = swap(jnp.moveaxis(labels, 1, 0), "brick")
    labels = jnp.moveaxis(labels, 0, 1).reshape(views, places)

    low = coeffs.astype(BF)
    patterns = []
    for v in range(views):
        part = dot(low, basis[v]).astype(BF)
        part = swap(bins_to_front(part, modes), "mode")
        patterns.append(jnp.sum(part.astype(F32), 0))

    target = swap(
        jnp.moveaxis(measured.reshape(views, -1, modes, mine), 2, 0), "mode"
    )
    target = jnp.moveaxis(target, 0, 1).reshape(views, rays, mine)

    share = views * mine // peers
    view_here, bin_here = (brick * share) // mine, (brick * share) % mine
    picked = lax.dynamic_index_in_dim(basis, view_here, 0, keepdims=False)
    picked = picked.reshape(-1, modes, mine)
    picked = lax.dynamic_slice_in_dim(picked, bin_here, share, 2)
    picked = picked.reshape(-1, modes * share)
    gram = [dot(picked, basis[u], ((0,), (0,))).astype(BF) for u in range(views)]
    gram = jnp.concatenate(gram, 1).reshape(modes, share, views * bins)
    gram = jnp.sum(swap(gram, "mode").astype(F32), 0).astype(BF)
    gram = lax.all_gather(gram, "brick", axis=0, tiled=True)

    spread, selector = [], []
    for v in range(views):
        source, used, _ = tables[v]
        moved = weights[v][source]
        moved = jnp.where(used[:, None, None] > 0, moved, jnp.zeros_like(moved))
        spread.append(moved.reshape(places * ray_block, voxels))
        row = jnp.arange(rays, dtype=jnp.int32)
        col = jnp.arange(places * ray_block, dtype=jnp.int32)
        label_row = jnp.repeat(labels[v], ray_block)
        selector.append(
            (label_row[None, :] * ray_block + col[None, :] % ray_block == row[:, None]).astype(BF)
        )

    def sweep(v, pattern):
        sent = dot(spread[v], pattern.astype(BF)).astype(BF)
        arrived = swap(sent.reshape(peers, -1, mine), "brick").reshape(-1, mine)
        residual = dot(selector[v], arrived) - target[v]
        back = dot(selector[v], residual.astype(BF), ((0,), (0,))).astype(BF)
        back = swap(back.reshape(peers, -1, mine), "brick").reshape(-1, mine)
        change = dot(spread[v], back, ((0,), (0,))).astype(BF)
        return residual, lax.all_gather(change, "mode", axis=0)

    first = [sweep(v, patterns[v]) for v in range(views)]
    gram = gram.reshape(views, mine, views, modes, mine)
    changes = [f[1] for f in first]
    later = []
    for v in range(views):
        step = sum(
            dot(changes[u][m], gram[v, :, u, m, :], ((1,), (1,)))
            for u in range(views)
            for m in range(modes)
        )
        later.append(patterns[v] - LEARN_RATE * step)

    def update(coeffs, changes):
        step = sum(
            dot(changes[u][m], basis[u][:, m * mine : (m + 1) * mine], ((1,), (1,)))
            for u in range(views)
            for m in range(modes)
        )
        return coeffs - LEARN_RATE * step

    coeffs = update(coeffs, changes)
    second = [sweep(v, later[v]) for v in range(views)]
    coeffs = update(coeffs, [s[1] for s in second])

    out = jnp.stack([s[0] for s in second], 0).reshape(views, modes, -1, mine)
    out = swap(jnp.moveaxis(out, 1, 0), "mode")
    out = jnp.moveaxis(out, 0, 2).reshape(views, -1, bins)
    return coeffs, out


def solution(mesh):
    return jax.shard_map(
        shards,
        mesh=mesh,
        in_specs=(
            P("brick", "mode"),
            P(None, "brick", None, None),
            P(None, "brick", None),
            P(None, "brick"),
            P(None, "mode", None),
            P(None, ("brick", "mode"), None),
        ),
        out_specs=(P("brick", "mode"), P(None, ("brick", "mode"), None)),
        check_vma=False,
    )
```

```python
import functools

import jax
import jax.numpy as jnp
from jax import lax
from jax.experimental import pallas as pl
from jax.experimental.pallas import tpu as pltpu
from jax.sharding import PartitionSpec as P

BLK_DEV = 8
LEARN_RATE = 0.2
BF = jnp.bfloat16
F32 = jnp.float32
MESH = pl.DeviceIdType.MESH


def dot(a, b):
    return jnp.dot(a, b, preferred_element_type=F32)


def slot_tables(owner_list, offset_list, peer_count, capacity):
    slots = owner_list.shape[0]
    order = jnp.arange(slots, dtype=jnp.int32)
    same = owner_list[:, None] == owner_list[None, :]
    earlier = jnp.sum((same & (order[None, :] < order[:, None])).astype(jnp.int32), 1)
    places = owner_list * capacity + earlier
    hits = places[None, :] == jnp.arange(peer_count * capacity, dtype=jnp.int32)[:, None]
    source = slots + jnp.sum(jnp.where(hits, order[None, :] - slots, 0), 1)
    labels = BLK_DEV + jnp.sum(jnp.where(hits, offset_list[None, :] - BLK_DEV, 0), 1)
    return source, places, labels


def kernel(
    peers,
    modes,
    cap,
    source,
    places,
    label_out,
    picked,
    coeffs_hbm,
    weights_hbm,
    basis_hbm,
    measured_hbm,
    coeffs_out,
    residual_out,
    coef,
    low,
    basis,
    weight,
    chunk,
    target,
    qsend,
    qrel,
    qrecv,
    pattern,
    qlow,
    proj,
    fsend,
    frecv,
    ray,
    bsend,
    brecv0,
    brecv1,
    back,
    back_t,
    change,
    select,
    gram,
    gpart,
    grecv,
    label_in,
    label_s,
    result,
    collected,
    load_sem,
    local_sem,
    gs_sem,
    gr_sem,
    ts_sem,
    tr_sem,
    qs_sem,
    qr_sem,
    as_sem,
    ar_sem,
    rs_sem,
    rr_sem,
    all_s,
    all_r,
):
    brecv = (brecv0, brecv1)
    brick, mode = lax.axis_index("brick"), lax.axis_index("mode")
    right, left, far = [lax.rem(mode + k, modes) for k in (1, modes - 1, 2)]
    views, entries, voxels = weights_hbm.shape
    slots, ray_block = proj.shape[0] - 1, proj.shape[1]
    here, bins = basis.shape[1], basis.shape[2]
    mine = bins // modes
    places_n = peers * cap
    rays = BLK_DEV * ray_block
    tile = min(256, voxels)
    half, hm = voxels // 2, mine // 2
    share = gpart.shape[0] // modes

    def aligned(i, n):
        return pl.ds(pl.multiple_of(i * n, n), n)

    def to_mode(src, dst, s, r, peer):
        copy = pltpu.make_async_remote_copy(
            src_ref=src, dst_ref=dst, send_sem=s, recv_sem=r,
            device_id={"mode": peer}, device_id_type=MESH,
        )
        copy.start()

    def await_bytes(ref, sem):
        pltpu.make_async_copy(ref, ref, sem).wait()

    def to_bricks(src_of, dst, index):
        def body(k, carry):
            peer = lax.rem(brick + k, peers)
            copy = pltpu.make_async_remote_copy(
                src_ref=src_of(peer), dst_ref=dst, send_sem=all_s.at[index],
                recv_sem=all_r.at[index], device_id={"brick": peer}, device_id_type=MESH,
            )
            copy.start()
            return carry

        lax.fori_loop(1, peers, body, 0)

    loads = [
        pltpu.make_async_copy(basis_hbm, basis, load_sem.at[0]),
        pltpu.make_async_copy(coeffs_hbm, coef, load_sem.at[1]),
        pltpu.make_async_copy(weights_hbm.at[0], weight.at[0], load_sem.at[2]),
        pltpu.make_async_copy(weights_hbm.at[1], weight.at[1], load_sem.at[3]),
    ]
    loads += [
        pltpu.make_async_copy(
            measured_hbm.at[:, :, pl.ds(m * mine, mine)], chunk.at[m], load_sem.at[4 + m]
        )
        for m in range(modes)
    ]
    for load in loads:
        load.start()
    barrier = pltpu.get_barrier_semaphore()

    def greet(k, carry):
        pl.semaphore_signal(
            barrier, inc=1, device_id={"brick": lax.rem(brick + k, peers)}, device_id_type=MESH
        )
        return carry

    lax.fori_loop(1, peers, greet, 0)
    for k in range(1, modes):
        pl.semaphore_signal(
            barrier, inc=1, device_id={"mode": lax.rem(mode + k, modes)}, device_id_type=MESH
        )
    proj[slots] = jnp.zeros(proj.shape[1:], BF)
    ray[BLK_DEV] = jnp.zeros(ray.shape[1:], BF)
    loads[0].wait()
    for u in range(views):
        gpart[:, u * bins : (u + 1) * bins] = dot(picked[...], basis[u]).astype(BF)
    loads[1].wait()

    def round_low(i, carry):
        low[aligned(i, tile), :] = coef[aligned(i, tile), :].astype(BF)
        return carry

    lax.fori_loop(0, voxels // tile, round_low, 0)
    pl.semaphore_wait(barrier, peers - 1 + modes - 1)

    for k in range(1, modes):
        peer = lax.rem(mode + k, modes)
        to_mode(gpart.at[aligned(peer, share)], grecv.at[k - 1], gs_sem.at[k], gr_sem.at[k], peer)
    to_bricks(lambda peer: label_out.at[peer], label_in.at[brick], 0)
    pltpu.make_async_copy(label_out.at[brick], label_in.at[brick], local_sem.at[0]).start()

    def partial_pattern(v, slot, m):
        def body(i, carry):
            rows = aligned(i, tile)
            value = dot(low[rows, :], basis[v, :, aligned(m, mine)])
            if slot is None:
                pattern[v, rows, :] = value
            else:
                qsend[v, slot, rows, :] = value.astype(BF)
            return carry

        lax.fori_loop(0, voxels // tile, body, 0)

    lower, upper = pl.ds(0, half), pl.ds(half, half)

    def scatter_start(v):
        partial_pattern(v, 0, far)
        to_mode(qsend.at[v, 0, upper], qrel.at[v, 0], qs_sem.at[v, 0], qr_sem.at[v, 0], right)
        to_mode(qsend.at[v, 0, lower], qrel.at[v, 1], qs_sem.at[v, 1], qr_sem.at[v, 1], left)
        partial_pattern(v, 1, right)
        to_mode(
            qsend.at[v, 1, lower], qrecv.at[v, 0, lower], qs_sem.at[v, 2], qr_sem.at[v, 2], right
        )
        partial_pattern(v, 2, left)
        to_mode(
            qsend.at[v, 2, upper], qrecv.at[v, 1, upper], qs_sem.at[v, 3], qr_sem.at[v, 3], left
        )
        partial_pattern(v, None, mode)

    def scatter_relay(v):
        for k, (slot, start, part, peer) in enumerate(((1, half, upper, right), (2, 0, lower, left))):
            await_bytes(qrel.at[v, k], qr_sem.at[v, k])

            def body(i, carry, k=k, slot=slot, start=start):
                rows = pl.ds(pl.multiple_of(start + i * (tile // 2), tile // 2), tile // 2)
                given = qrel[v, k, aligned(i, tile // 2), :].astype(F32)
                qsend[v, slot, rows, :] = (qsend[v, slot, rows, :].astype(F32) + given).astype(BF)
                return carry

            lax.fori_loop(0, half // (tile // 2), body, 0)
            to_mode(
                qsend.at[v, slot, part], qrecv.at[v, k, part],
                qs_sem.at[v, 4 + k], qr_sem.at[v, 4 + k], peer,
            )

    def scatter_end(v):
        await_bytes(qrecv.at[v, 0, lower], qr_sem.at[v, 2])
        await_bytes(qrecv.at[v, 1, upper], qr_sem.at[v, 3])
        await_bytes(qrecv.at[v, 0, upper], qr_sem.at[v, 4])
        await_bytes(qrecv.at[v, 1, lower], qr_sem.at[v, 5])

        def body(i, carry):
            rows = aligned(i, tile)
            total = pattern[v, rows, :] + qrecv[v, 0, rows, :].astype(F32)
            total = total + qrecv[v, 1, rows, :].astype(F32)
            pattern[v, rows, :] = total
            qlow[v, rows, :] = total.astype(BF)
            return carry

        lax.fori_loop(0, voxels // tile, body, 0)

    scatter_start(0)
    own = aligned(mode, share)
    for k in range(1, modes):
        await_bytes(grecv.at[k - 1], gr_sem.at[k])
    total = gpart[own, :].astype(F32)
    for k in range(1, modes):
        total = total + grecv[k - 1].astype(F32)
    gram[aligned(brick, share), :] = total.astype(BF)
    to_bricks(lambda peer: gram.at[aligned(brick, share)], gram.at[aligned(brick, share)], 1)
    for m in range(modes):
        loads[4 + m].wait()
    for k in range(1, modes):
        peer = lax.rem(mode + k, modes)
        to_mode(chunk.at[peer], target.at[mode], ts_sem.at[k], tr_sem.at[k], peer)
    pltpu.make_async_copy(chunk.at[mode], target.at[mode], local_sem.at[1]).start()
    scatter_relay(0)
    scatter_start(1)

    await_bytes(label_in.at[pl.ds(0, peers - 1)], all_r.at[0])
    pltpu.make_async_copy(label_out.at[brick], label_in.at[brick], local_sem.at[0]).wait()
    table = pltpu.make_async_copy(label_in, label_s, local_sem.at[2])
    table.start()
    table.wait()
    group = 128 // ray_block

    def build(t, carry):
        row = lax.broadcasted_iota(jnp.int32, (rays, 128), 0)
        lane = lax.broadcasted_iota(jnp.int32, (rays, 128), 1)
        for v in range(views):
            want = jnp.zeros((rays, 128), jnp.int32)
            for g in range(group):
                entry = t * group + g
                label = label_s[entry // cap, 0, v * cap + entry % cap]
                inside = (lane >= g * ray_block) & (lane < (g + 1) * ray_block)
                want = jnp.where(inside, label * ray_block + lane - g * ray_block, want)
            select[v, :, aligned(t, 128)] = jnp.where(want == row, 1.0, 0.0).astype(BF)
        return carry

    lax.fori_loop(0, places_n // group, build, 0)

    def forward(s, v):
        def body(i, carry):
            value = dot(weight[v, aligned(i, rays), :], qlow[v]).astype(BF)
            proj[pl.ds(i * BLK_DEV, BLK_DEV)] = value.reshape(BLK_DEV, ray_block, mine)
            return carry

        lax.fori_loop(0, entries // rays, body, 0)
        if s:
            await_bytes(fsend.at[v, pl.ds(0, places_n - cap)], all_s.at[2 + v])

        def pack(i, carry):
            fsend[v, i] = proj[source[v, i]]
            return carry

        lax.fori_loop(0, places_n, pack, 0, unroll=8)
        where = pl.ds(brick * cap, cap)
        to_bricks(
            lambda peer: fsend.at[v, pl.ds(peer * cap, cap)], frecv.at[v, where], 2 + 4 * s + v
        )
        pltpu.make_async_copy(fsend.at[v, where], frecv.at[v, where], local_sem.at[3 + v]).start()

    def reflect(s, v):
        where = pl.ds(brick * cap, cap)
        await_bytes(frecv.at[v, pl.ds(0, places_n - cap)], all_r.at[2 + 4 * s + v])
        pltpu.make_async_copy(fsend.at[v, where], frecv.at[v, where], local_sem.at[3 + v]).wait()
        goal = jnp.concatenate([target[m, v] for m in range(modes)], 0)
        value = dot(select[v], frecv[v].reshape(places_n * ray_block, mine)) - goal
        if s:
            result[:, v] = value.reshape(modes, rays // modes, mine)
            await_bytes(bsend.at[v, pl.ds(0, places_n - cap)], all_s.at[4 + v])
        ray[pl.ds(0, BLK_DEV)] = value.astype(BF).reshape(BLK_DEV, ray_block, mine)

        def answer(p, carry):
            for c in range(cap):
                bsend[v, p * cap + c] = ray[label_s[p, 0, v * cap + c]]
            return carry

        lax.fori_loop(0, peers, answer, 0, unroll=4)
        to_bricks(
            lambda peer: bsend.at[v, pl.ds(peer * cap, cap)], brecv[v].at[where], 4 + 4 * s + v
        )
        pltpu.make_async_copy(bsend.at[v, where], brecv[v].at[where], local_sem.at[5 + v]).start()

    def adjoint(s, v):
        where = pl.ds(brick * cap, cap)
        await_bytes(brecv[v].at[pl.ds(0, places_n - cap)], all_r.at[4 + 4 * s + v])
        pltpu.make_async_copy(bsend.at[v, where], brecv[v].at[where], local_sem.at[5 + v]).wait()

        def unpack(i, carry):
            back[i] = brecv[v][places[v, i]]
            return carry

        lax.fori_loop(0, slots, unpack, 0, unroll=8 if slots % 8 == 0 else 1)

        def turn(i, carry):
            piece = back[pl.ds(i * BLK_DEV, BLK_DEV)].reshape(rays, mine).astype(F32)
            back_t[:, aligned(i, rays)] = piece.T.astype(BF)
            return carry

        lax.fori_loop(0, entries // rays, turn, 0)

        def body(j, carry):
            cols = aligned(j, tile)
            change[s, v, aligned(mode, mine), cols] = dot(back_t[...], weight[v, :, cols]).astype(BF)
            return carry

        lax.fori_loop(0, voxels // tile, body, 0)
        for k, (skip, peer) in enumerate(((hm, right), (0, right), (0, left), (hm, left))):
            part = change.at[s, v, pl.ds(pl.multiple_of(mode * mine + skip, hm), hm)]
            to_mode(part, part, as_sem.at[s, v, k], ar_sem.at[s, v, k], peer)

    def gather_relay(s, v):
        for k, (giver, skip, peer) in enumerate(((left, hm, right), (right, 0, left))):
            part = change.at[s, v, pl.ds(pl.multiple_of(giver * mine + skip, hm), hm)]
            await_bytes(part, ar_sem.at[s, v, 2 * k])
            to_mode(part, part, as_sem.at[s, v, 4 + k], ar_sem.at[s, v, 4 + k], peer)

    def gather_end(s, v):
        for k in (1, 3, 4, 5):
            await_bytes(change.at[s, v, pl.ds(0, hm)], ar_sem.at[s, v, k])

    def renew(u):
        def body(j, carry):
            cols = aligned(j, tile)
            step = dot(gram[:, u * bins : (u + 1) * bins], change[0, u, :, cols]).T
            for v in range(views):
                value = pattern[v, cols, :] - LEARN_RATE * step[:, v * mine : (v + 1) * mine]
                pattern[v, cols, :] = value
                if u == views - 1:
                    qlow[v, cols, :] = value.astype(BF)
            return carry

        lax.fori_loop(0, voxels // tile, body, 0)

    def update(s, us, out):
        def body(j, carry):
            cols = aligned(j, tile)
            step = sum(dot(basis[u], change[s, u, :, cols]) for u in us).T
            coef[cols, :] = coef[cols, :] - LEARN_RATE * step
            if out:
                pltpu.make_async_copy(
                    coef.at[cols], coeffs_out.at[cols], load_sem.at[j]
                ).start()
            return carry

        lax.fori_loop(0, voxels // tile, body, 0)

    scatter_end(0)
    loads[2].wait()
    forward(0, 0)
    scatter_relay(1)
    for k in range(1, modes):
        await_bytes(target.at[0], tr_sem.at[k])
    pltpu.make_async_copy(chunk.at[mode], target.at[mode], local_sem.at[1]).wait()
    reflect(0, 0)
    scatter_end(1)
    loads[3].wait()
    forward(0, 1)
    adjoint(0, 0)
    reflect(0, 1)
    gather_relay(0, 0)
    await_bytes(gram.at[pl.ds(0, gram.shape[0] - share)], all_r.at[1])
    gather_end(0, 0)
    renew(0)
    adjoint(0, 1)
    gather_relay(0, 1)
    gather_end(0, 1)
    renew(1)
    forward(1, 0)
    forward(1, 1)
    update(0, range(views), False)
    reflect(1, 0)
    reflect(1, 1)
    for k in range(1, modes):
        peer = lax.rem(mode + k, modes)
        to_mode(result.at[peer], collected.at[mode], rs_sem.at[k], rr_sem.at[k], peer)
    pltpu.make_async_copy(result.at[mode], collected.at[mode], local_sem.at[7]).start()
    adjoint(1, 0)
    gather_relay(1, 0)
    adjoint(1, 1)
    gather_end(1, 0)
    update(1, (0,), False)
    gather_relay(1, 1)
    for k in range(1, modes):
        await_bytes(collected.at[0], rr_sem.at[k])
    pltpu.make_async_copy(result.at[mode], collected.at[mode], local_sem.at[7]).wait()
    writes = [
        pltpu.make_async_copy(
            collected.at[m], residual_out.at[:, :, pl.ds(m * mine, mine)], load_sem.at[4 + m]
        )
        for m in range(modes)
    ]
    for write in writes:
        write.start()
    gather_end(1, 1)
    update(1, (1,), True)

    for k in range(1, modes):
        await_bytes(grecv.at[0], gs_sem.at[k])
        await_bytes(chunk.at[0], ts_sem.at[k])
        await_bytes(result.at[0], rs_sem.at[k])
    for v in range(views):
        for k in range(6):
            await_bytes(qrel.at[0, 0], qs_sem.at[v, k])
            for s in range(2):
                await_bytes(change.at[0, 0, pl.ds(0, hm)], as_sem.at[s, v, k])
        await_bytes(fsend.at[v, pl.ds(0, places_n - cap)], all_s.at[6 + v])
        await_bytes(bsend.at[v, pl.ds(0, places_n - cap)], all_s.at[8 + v])
    await_bytes(label_in.at[pl.ds(0, peers - 1)], all_s.at[0])
    await_bytes(gram.at[pl.ds(0, gram.shape[0] - share)], all_s.at[1])
    for write in writes:
        write.wait()

    def drain(j, carry):
        cols = aligned(j, tile)
        pltpu.make_async_copy(coef.at[cols], coeffs_out.at[cols], load_sem.at[j]).wait()
        return carry

    lax.fori_loop(0, voxels // tile, drain, 0)


def shards(coeffs, weights, owners, offsets, basis, measured):
    peers, modes = lax.axis_size("brick"), lax.axis_size("mode")
    views, slots, ray_block, voxels = weights.shape
    cap = max(2, slots // peers + 1)
    here, bins = basis.shape[1:]
    mine = bins // modes
    places_n = peers * cap
    rays = BLK_DEV * ray_block
    brick = lax.axis_index("brick")

    source, places, labels = jax.vmap(lambda o, f: slot_tables(o, f, peers, cap))(
        owners[:, :, 0], offsets
    )
    labels = jnp.moveaxis(labels.reshape(views, peers, cap), 1, 0).reshape(peers, views * cap)
    labels = jnp.pad(labels, ((0, 0), (0, 128 - views * cap))).reshape(peers, 1, 128)

    share = views * mine // peers
    view_here, bin_here = (brick * share) // mine, (brick * share) % mine
    picked = lax.dynamic_index_in_dim(basis, view_here, 0, keepdims=False)
    picked = lax.dynamic_slice_in_dim(picked.reshape(here, modes, mine), bin_here, share, 2)
    picked = picked.reshape(here, modes * share).T

    smem = pl.BlockSpec(memory_space=pltpu.SMEM)
    vmem = pl.BlockSpec(memory_space=pltpu.VMEM)
    anywhere = pl.BlockSpec(memory_space=pl.ANY)
    dma = pltpu.SemaphoreType.DMA
    blocks = (views, places_n, ray_block, mine)
    coeffs, residual = pl.pallas_call(
        functools.partial(kernel, peers, modes, cap),
        out_shape=(
            jax.ShapeDtypeStruct(coeffs.shape, F32),
            jax.ShapeDtypeStruct(measured.shape, F32),
        ),
        in_specs=[smem, smem, vmem, vmem] + [anywhere] * 4,
        out_specs=(anywhere, anywhere),
        scratch_shapes=[
            pltpu.VMEM(coeffs.shape, F32),
            pltpu.VMEM(coeffs.shape, BF),
            pltpu.VMEM(basis.shape, BF),
            pltpu.VMEM((views, slots * ray_block, voxels), BF),
            pltpu.VMEM((modes, views, rays // modes, mine), F32),
            pltpu.VMEM((modes, views, rays // modes, mine), F32),
            pltpu.VMEM((views, 3, voxels, mine), BF),
            pltpu.VMEM((views, 2, voxels // 2, mine), BF),
            pltpu.VMEM((views, 2, voxels, mine), BF),
            pltpu.VMEM((views, voxels, mine), F32),
            pltpu.VMEM((views, voxels, mine), BF),
            pltpu.VMEM((slots + 1, ray_block, mine), BF),
            pltpu.VMEM(blocks, BF),
            pltpu.VMEM(blocks, BF),
            pltpu.VMEM((BLK_DEV + 1, ray_block, mine), BF),
            pltpu.VMEM(blocks, BF),
            pltpu.VMEM(blocks[1:], BF),
            pltpu.VMEM(blocks[1:], BF),
            pltpu.VMEM((slots, ray_block, mine), BF),
            pltpu.VMEM((mine, slots * ray_block), BF),
            pltpu.VMEM((2, views, bins, voxels), BF),
            pltpu.VMEM((views, rays, places_n * ray_block), BF),
            pltpu.VMEM((views * mine, views * bins), BF),
            pltpu.VMEM((modes * share, views * bins), BF),
            pltpu.VMEM((modes - 1, share, views * bins), BF),
            pltpu.VMEM((peers, 1, 128), jnp.int32),
            pltpu.SMEM((peers, 1, 128), jnp.int32),
            pltpu.VMEM((modes, views, rays // modes, mine), F32),
            pltpu.VMEM((modes, views, rays // modes, mine), F32),
            dma((8,)),
            dma((8,)),
            dma((4,)),
            dma((4,)),
            dma((4,)),
            dma((4,)),
            dma((2, 6)),
            dma((2, 6)),
            dma((2, 2, 6)),
            dma((2, 2, 6)),
            dma((4,)),
            dma((4,)),
            dma((10,)),
            dma((10,)),
        ],
        compiler_params=pltpu.CompilerParams(
            collective_id=0, has_side_effects=True, vmem_limit_bytes=67043328
        ),
    )(source, places, labels, picked, coeffs, weights.reshape(views, -1, voxels), basis, measured)
    return coeffs, residual


def solution(mesh):
    return jax.shard_map(
        shards,
        mesh=mesh,
        in_specs=(
            P("brick", "mode"),
            P(None, "brick", None, None),
            P(None, "brick", None),
            P(None, "brick"),
            P(None, "mode", None),
            P(None, ("brick", "mode"), None),
        ),
        out_specs=(P("brick", "mode"), P(None, ("brick", "mode"), None)),
        check_vma=False,
    )
```

```python
import functools

import jax
import jax.numpy as jnp
from jax import lax
from jax.experimental import pallas as pl
from jax.experimental.pallas import tpu as pltpu
from jax.sharding import PartitionSpec as P

BLK_DEV = 8
LEARN_RATE = 0.2
BF = jnp.bfloat16
F32 = jnp.float32
MESH = pl.DeviceIdType.MESH


def dot(a, b):
    return jnp.dot(a, b, preferred_element_type=F32)


def slot_tables(owner_list, offset_list, peer_count, capacity):
    slots = owner_list.shape[0]
    order = jnp.arange(slots, dtype=jnp.int32)
    same = owner_list[:, None] == owner_list[None, :]
    earlier = jnp.sum((same & (order[None, :] < order[:, None])).astype(jnp.int32), 1)
    places = owner_list * capacity + earlier
    hits = places[None, :] == jnp.arange(peer_count * capacity, dtype=jnp.int32)[:, None]
    source = slots + jnp.sum(jnp.where(hits, order[None, :] - slots, 0), 1)
    labels = BLK_DEV + jnp.sum(jnp.where(hits, offset_list[None, :] - BLK_DEV, 0), 1)
    return source, places, labels


def kernel(
    peers,
    modes,
    cap,
    source,
    places,
    label_out,
    picked,
    coeffs_hbm,
    weights_hbm,
    basis_hbm,
    measured_hbm,
    coeffs_out,
    residual_out,
    coef,
    low,
    basis,
    weight,
    chunk,
    target,
    qsend,
    qrel,
    qrecv,
    pattern,
    qlow,
    proj,
    fsend,
    frecv,
    ray,
    bsend,
    brecv0,
    brecv1,
    brecv2,
    brecv3,
    back,
    back_t,
    change,
    select,
    gram,
    gpart,
    grecv,
    label_in,
    label_s,
    result,
    collected,
    load_sem,
    local_sem,
    gs_sem,
    gr_sem,
    ts_sem,
    tr_sem,
    qs_sem,
    qr_sem,
    as_sem,
    ar_sem,
    rs_sem,
    rr_sem,
    all_s,
    all_r,
    write_sem,
):
    brecv = (brecv0, brecv1, brecv2, brecv3)
    brick, mode = lax.axis_index("brick"), lax.axis_index("mode")
    right, left, far = [lax.rem(mode + k, modes) for k in (1, modes - 1, 2)]
    views, entries, voxels = weights_hbm.shape
    slots, ray_block = proj.shape[0] - 1, proj.shape[1]
    here, bins = basis.shape[1], basis.shape[2]
    mine = bins // modes
    places_n = peers * cap
    rays = BLK_DEV * ray_block
    tile = min(256, voxels)
    width = mine // 2
    half, hm = voxels // 2, width // 2
    share = gpart.shape[0] // modes

    def aligned(i, n):
        return pl.ds(pl.multiple_of(i * n, n), n)

    def to_mode(src, dst, s, r, peer):
        copy = pltpu.make_async_remote_copy(
            src_ref=src, dst_ref=dst, send_sem=s, recv_sem=r,
            device_id={"mode": peer}, device_id_type=MESH,
        )
        copy.start()

    def await_bytes(ref, sem):
        pltpu.make_async_copy(ref, ref, sem).wait()

    def to_bricks(src_of, dst, index):
        def body(k, carry):
            peer = lax.rem(brick + k, peers)
            copy = pltpu.make_async_remote_copy(
                src_ref=src_of(peer), dst_ref=dst, send_sem=all_s.at[index],
                recv_sem=all_r.at[index], device_id={"brick": peer}, device_id_type=MESH,
            )
            copy.start()
            return carry

        lax.fori_loop(1, peers, body, 0)

    loads = [
        pltpu.make_async_copy(basis_hbm, basis, load_sem.at[0]),
        pltpu.make_async_copy(coeffs_hbm, coef, load_sem.at[1]),
        pltpu.make_async_copy(weights_hbm.at[0], weight.at[0], load_sem.at[2]),
        pltpu.make_async_copy(weights_hbm.at[1], weight.at[1], load_sem.at[3]),
    ]
    loads += [
        pltpu.make_async_copy(
            measured_hbm.at[:, :, pl.ds(m * mine, mine)], chunk.at[m], load_sem.at[4 + m]
        )
        for m in range(modes)
    ]
    for load in loads:
        load.start()
    barrier = pltpu.get_barrier_semaphore()

    def greet(k, carry):
        pl.semaphore_signal(
            barrier, inc=1, device_id={"brick": lax.rem(brick + k, peers)}, device_id_type=MESH
        )
        return carry

    lax.fori_loop(1, peers, greet, 0)
    for k in range(1, modes):
        pl.semaphore_signal(
            barrier, inc=1, device_id={"mode": lax.rem(mode + k, modes)}, device_id_type=MESH
        )
    proj[slots] = jnp.zeros(proj.shape[1:], BF)
    ray[BLK_DEV] = jnp.zeros(ray.shape[1:], BF)
    loads[0].wait()
    for u in range(views):
        gpart[:, u * bins : (u + 1) * bins] = dot(picked[...], basis[u]).astype(BF)
    loads[1].wait()

    def round_low(i, carry):
        low[aligned(i, tile), :] = coef[aligned(i, tile), :].astype(BF)
        return carry

    lax.fori_loop(0, voxels // tile, round_low, 0)
    lower, upper = pl.ds(0, half), pl.ds(half, half)

    def partial_patterns(v):
        def body(i, carry):
            rows = aligned(i, tile)
            for slot, m in ((0, far), (1, right), (2, left)):
                value = dot(low[rows, :], basis[v, :, aligned(m, mine)]).astype(BF)
                for h in range(2):
                    qsend[v, slot, h, rows, :] = value[:, h * width : (h + 1) * width]
            return carry

        lax.fori_loop(0, voxels // tile, body, 0)

    def own_pattern(v):
        def body(i, carry):
            rows = aligned(i, tile)
            value = dot(low[rows, :], basis[v, :, aligned(mode, mine)])
            for h in range(2):
                pattern[2 * v + h, rows, :] = value[:, h * width : (h + 1) * width]
            return carry

        lax.fori_loop(0, voxels // tile, body, 0)

    def scatter_send(c):
        v, h = c // 2, c % 2
        for k, (slot, part, dst, peer) in enumerate(
            (
                (0, upper, qrel.at[c, 0], right),
                (0, lower, qrel.at[c, 1], left),
                (1, lower, qrecv.at[c, 0, lower], right),
                (2, upper, qrecv.at[c, 1, upper], left),
            )
        ):
            to_mode(qsend.at[v, slot, h, part], dst, qs_sem.at[c, k], qr_sem.at[c, k], peer)

    def scatter_relay(c):
        v, h = c // 2, c % 2
        for k, (slot, start, part, peer) in enumerate(((1, half, upper, right), (2, 0, lower, left))):
            await_bytes(qrel.at[c, k], qr_sem.at[c, k])

            def body(i, carry, k=k, slot=slot, start=start):
                rows = pl.ds(pl.multiple_of(start + i * (tile // 2), tile // 2), tile // 2)
                given = qrel[c, k, aligned(i, tile // 2), :].astype(F32)
                total = qsend[v, slot, h, rows, :].astype(F32) + given
                qsend[v, slot, h, rows, :] = total.astype(BF)
                return carry

            lax.fori_loop(0, half // (tile // 2), body, 0)
            to_mode(
                qsend.at[v, slot, h, part], qrecv.at[c, k, part],
                qs_sem.at[c, 4 + k], qr_sem.at[c, 4 + k], peer,
            )

    def scatter_end(c):
        for k, part in ((2, lower), (3, upper), (4, upper), (5, lower)):
            await_bytes(qrecv.at[c, 0, part], qr_sem.at[c, k])

        def body(i, carry):
            rows = aligned(i, tile)
            total = pattern[c, rows, :] + qrecv[c, 0, rows, :].astype(F32)
            total = total + qrecv[c, 1, rows, :].astype(F32)
            pattern[c, rows, :] = total
            qlow[c, rows, :] = total.astype(BF)
            return carry

        lax.fori_loop(0, voxels // tile, body, 0)

    def share_gram():
        own = aligned(mode, share)
        for k in range(1, modes):
            await_bytes(grecv.at[k - 1], gr_sem.at[k])
        total = gpart[own, :].astype(F32)
        for k in range(1, modes):
            total = total + grecv[k - 1].astype(F32)
        gram[aligned(brick, share), :] = total.astype(BF)
        rows = gram.at[aligned(brick, share)]

        def body(k, carry):
            peer = lax.rem(brick + 2 * k, peers)
            copy = pltpu.make_async_remote_copy(
                src_ref=rows, dst_ref=rows, send_sem=all_s.at[1],
                recv_sem=all_r.at[1], device_id={"brick": peer}, device_id_type=MESH,
            )
            copy.start()
            return carry

        lax.fori_loop(1, peers // 2, body, 0)

    def hand_gram():
        await_bytes(gram.at[pl.ds(0, (peers // 2 - 1) * share)], all_r.at[1])
        core = lax.rem(brick, 2)
        twin = brick + 1 - 2 * core

        def body(k, carry):
            rows = gram.at[aligned(2 * k + core, share)]
            copy = pltpu.make_async_remote_copy(
                src_ref=rows, dst_ref=rows, send_sem=all_s.at[2],
                recv_sem=all_r.at[2], device_id={"brick": twin}, device_id_type=MESH,
            )
            copy.start()
            return carry

        lax.fori_loop(0, peers // 2, body, 0)

    def share_measured(v):
        for k in range(1, modes):
            peer = lax.rem(mode + k, modes)
            to_mode(
                chunk.at[peer, v], target.at[mode, v], ts_sem.at[v, k], tr_sem.at[v, k], peer
            )
        pltpu.make_async_copy(chunk.at[mode, v], target.at[mode, v], local_sem.at[1 + v]).start()

    def measured_end(v):
        for k in range(1, modes):
            await_bytes(target.at[0, v], tr_sem.at[v, k])
        pltpu.make_async_copy(chunk.at[mode, v], target.at[mode, v], local_sem.at[1 + v]).wait()

    def share_result(v):
        for k in range(1, modes):
            peer = lax.rem(mode + k, modes)
            to_mode(
                result.at[peer, v], collected.at[mode, v], rs_sem.at[v, k], rr_sem.at[v, k], peer
            )
        pltpu.make_async_copy(
            result.at[mode, v], collected.at[mode, v], local_sem.at[1 + v]
        ).start()

    def result_end(v):
        for k in range(1, modes):
            await_bytes(collected.at[0, v], rr_sem.at[v, k])
        pltpu.make_async_copy(
            result.at[mode, v], collected.at[mode, v], local_sem.at[1 + v]
        ).wait()

    group = 128 // ray_block

    def build_select():
        await_bytes(label_in.at[pl.ds(0, peers - 1)], all_r.at[0])
        pltpu.make_async_copy(label_out.at[brick], label_in.at[brick], local_sem.at[0]).wait()
        table = pltpu.make_async_copy(label_in, label_s, local_sem.at[0])
        table.start()
        table.wait()

        def build(t, carry):
            row = lax.broadcasted_iota(jnp.int32, (rays, 128), 0)
            lane = lax.broadcasted_iota(jnp.int32, (rays, 128), 1)
            for v in range(views):
                want = jnp.zeros((rays, 128), jnp.int32)
                for g in range(group):
                    entry = t * group + g
                    label = label_s[entry // cap, 0, v * cap + entry % cap]
                    inside = (lane >= g * ray_block) & (lane < (g + 1) * ray_block)
                    want = jnp.where(inside, label * ray_block + lane - g * ray_block, want)
                select[v, :, aligned(t, 128)] = jnp.where(want == row, 1.0, 0.0).astype(BF)
            return carry

        lax.fori_loop(0, places_n // group, build, 0)

    own_slots = pl.ds(brick * cap, cap)
    others = pl.ds(0, places_n - cap)

    def forward(s, c):
        v = c // 2

        def body(i, carry):
            value = dot(weight[v, aligned(i, rays), :], qlow[c]).astype(BF)
            proj[pl.ds(i * BLK_DEV, BLK_DEV)] = value.reshape(BLK_DEV, ray_block, width)
            return carry

        lax.fori_loop(0, entries // rays, body, 0)
        if s:
            await_bytes(fsend.at[c, others], all_s.at[3 + c])

        def pack(i, carry):
            fsend[c, i] = proj[source[v, i]]
            return carry

        lax.fori_loop(0, places_n, pack, 0, unroll=8)
        to_bricks(
            lambda peer: fsend.at[c, pl.ds(peer * cap, cap)], frecv.at[c, own_slots], 3 + 4 * s + c
        )
        pltpu.make_async_copy(
            fsend.at[c, own_slots], frecv.at[c, own_slots], local_sem.at[3 + c]
        ).start()

    def reflect(s, c):
        v, h = c // 2, c % 2
        lanes = slice(h * width, (h + 1) * width)
        await_bytes(frecv.at[c, others], all_r.at[3 + 4 * s + c])
        pltpu.make_async_copy(
            fsend.at[c, own_slots], frecv.at[c, own_slots], local_sem.at[3 + c]
        ).wait()
        goal = jnp.concatenate([target[m, v, :, lanes] for m in range(modes)], 0)
        value = dot(select[v], frecv[c].reshape(places_n * ray_block, width)) - goal
        if s:
            result[:, v, :, lanes] = value.reshape(modes, rays // modes, width)
            await_bytes(bsend.at[c, others], all_s.at[11 + c])
        ray[pl.ds(0, BLK_DEV)] = value.astype(BF).reshape(BLK_DEV, ray_block, width)

        def answer(p, carry):
            for k in range(cap):
                bsend[c, p * cap + k] = ray[label_s[p, 0, v * cap + k]]
            return carry

        lax.fori_loop(0, peers, answer, 0, unroll=4)
        to_bricks(
            lambda peer: bsend.at[c, pl.ds(peer * cap, cap)], brecv[c].at[own_slots], 11 + 4 * s + c
        )
        pltpu.make_async_copy(
            bsend.at[c, own_slots], brecv[c].at[own_slots], local_sem.at[7 + c]
        ).start()

    def adjoint(s, c):
        v, h = c // 2, c % 2
        await_bytes(brecv[c].at[others], all_r.at[11 + 4 * s + c])
        pltpu.make_async_copy(
            bsend.at[c, own_slots], brecv[c].at[own_slots], local_sem.at[7 + c]
        ).wait()

        def unpack(i, carry):
            back[i] = brecv[c][places[v, i]]
            return carry

        lax.fori_loop(0, slots, unpack, 0, unroll=8)

        def turn(i, carry):
            piece = back[pl.ds(i * BLK_DEV, BLK_DEV)].reshape(rays, width).astype(F32)
            back_t[:, aligned(i, rays)] = piece.T.astype(BF)
            return carry

        lax.fori_loop(0, entries // rays, turn, 0)
        rows = pl.ds(pl.multiple_of(mode * mine + h * width, width), width)

        def body(j, carry):
            cols = aligned(j, tile)
            change[s, v, rows, cols] = dot(back_t[...], weight[v, :, cols]).astype(BF)
            return carry

        lax.fori_loop(0, voxels // tile, body, 0)
        for k, (skip, peer) in enumerate(((hm, right), (0, right), (0, left), (hm, left))):
            part = change.at[
                s, v, pl.ds(pl.multiple_of(mode * mine + h * width + skip, hm), hm)
            ]
            to_mode(part, part, as_sem.at[s, c, k], ar_sem.at[s, c, k], peer)

    def gather_relay(s, c):
        v, h = c // 2, c % 2
        for k, (giver, skip, peer) in enumerate(((left, hm, right), (right, 0, left))):
            part = change.at[
                s, v, pl.ds(pl.multiple_of(giver * mine + h * width + skip, hm), hm)
            ]
            await_bytes(part, ar_sem.at[s, c, 2 * k])
            to_mode(part, part, as_sem.at[s, c, 4 + k], ar_sem.at[s, c, 4 + k], peer)

    def gather_end(s, c):
        for k in (1, 3, 4, 5):
            await_bytes(change.at[s, c // 2, pl.ds(0, hm)], ar_sem.at[s, c, k])

    def renew(u):
        def body(j, carry):
            cols = aligned(j, tile)
            step = dot(gram[:, u * bins : (u + 1) * bins], change[0, u, :, cols]).T
            for c in range(2 * views):
                value = pattern[c, cols, :] - LEARN_RATE * step[:, c * width : (c + 1) * width]
                pattern[c, cols, :] = value
                if u == views - 1:
                    qlow[c, cols, :] = value.astype(BF)
            return carry

        lax.fori_loop(0, voxels // tile, body, 0)

    def update(s, us, out):
        def body(j, carry):
            cols = aligned(j, tile)
            step = sum(dot(basis[u], change[s, u, :, cols]) for u in us).T
            coef[cols, :] = coef[cols, :] - LEARN_RATE * step
            if out:
                pltpu.make_async_copy(
                    coef.at[cols], coeffs_out.at[cols], load_sem.at[j]
                ).start()
            return carry

        lax.fori_loop(0, voxels // tile, body, 0)

    partial_patterns(0)
    own_pattern(0)
    pl.semaphore_wait(barrier, peers - 1 + modes - 1)

    for k in range(1, modes):
        peer = lax.rem(mode + k, modes)
        to_mode(gpart.at[aligned(peer, share)], grecv.at[k - 1], gs_sem.at[k], gr_sem.at[k], peer)
    to_bricks(lambda peer: label_out.at[peer], label_in.at[brick], 0)
    pltpu.make_async_copy(label_out.at[brick], label_in.at[brick], local_sem.at[0]).start()
    scatter_send(0)
    share_gram()
    for m in range(modes):
        loads[4 + m].wait()
    scatter_relay(0)
    share_measured(0)
    scatter_send(1)
    partial_patterns(1)
    own_pattern(1)
    loads[2].wait()
    scatter_end(0)
    forward(0, 0)
    build_select()
    scatter_relay(1)
    scatter_send(2)
    measured_end(0)
    reflect(0, 0)
    scatter_end(1)
    forward(0, 1)
    scatter_relay(2)
    share_measured(1)
    scatter_send(3)
    loads[3].wait()
    scatter_end(2)
    forward(0, 2)
    scatter_relay(3)
    adjoint(0, 0)
    reflect(0, 1)
    scatter_end(3)
    forward(0, 3)
    gather_relay(0, 0)
    measured_end(1)
    reflect(0, 2)
    hand_gram()
    adjoint(0, 1)
    reflect(0, 3)
    gather_relay(0, 1)
    adjoint(0, 2)
    gather_end(0, 0)
    gather_end(0, 1)
    await_bytes(gram.at[pl.ds(0, peers // 2 * share)], all_r.at[2])
    renew(0)
    gather_relay(0, 2)
    adjoint(0, 3)
    gather_relay(0, 3)
    gather_end(0, 2)
    gather_end(0, 3)
    renew(1)
    forward(1, 0)
    forward(1, 1)
    update(0, range(views), False)
    reflect(1, 0)
    forward(1, 2)
    reflect(1, 1)
    forward(1, 3)
    share_result(0)
    adjoint(1, 0)
    reflect(1, 2)
    gather_relay(1, 0)
    adjoint(1, 1)
    reflect(1, 3)
    share_result(1)
    gather_relay(1, 1)
    adjoint(1, 2)
    gather_relay(1, 2)
    adjoint(1, 3)
    gather_end(1, 0)
    gather_end(1, 1)
    update(1, (0,), False)
    gather_relay(1, 3)
    writes = []
    for v in range(views):
        result_end(v)
        writes += [
            pltpu.make_async_copy(
                collected.at[m, v],
                residual_out.at[v, :, pl.ds(m * mine, mine)],
                write_sem.at[v, m],
            )
            for m in range(modes)
        ]
    for write in writes:
        write.start()
    gather_end(1, 2)
    gather_end(1, 3)
    update(1, (1,), True)

    for k in range(1, modes):
        await_bytes(grecv.at[0], gs_sem.at[k])
        for v in range(views):
            await_bytes(chunk.at[0, v], ts_sem.at[v, k])
            await_bytes(result.at[0, v], rs_sem.at[v, k])
    for c in range(2 * views):
        for k in range(6):
            await_bytes(qrel.at[0, 0], qs_sem.at[c, k])
            for s in range(2):
                await_bytes(change.at[0, 0, pl.ds(0, hm)], as_sem.at[s, c, k])
        await_bytes(fsend.at[c, others], all_s.at[7 + c])
        await_bytes(bsend.at[c, others], all_s.at[15 + c])
    await_bytes(label_in.at[pl.ds(0, peers - 1)], all_s.at[0])
    await_bytes(gram.at[pl.ds(0, (peers // 2 - 1) * share)], all_s.at[1])
    await_bytes(gram.at[pl.ds(0, peers // 2 * share)], all_s.at[2])
    for write in writes:
        write.wait()

    def drain(j, carry):
        cols = aligned(j, tile)
        pltpu.make_async_copy(coef.at[cols], coeffs_out.at[cols], load_sem.at[j]).wait()
        return carry

    lax.fori_loop(0, voxels // tile, drain, 0)


def shards(coeffs, weights, owners, offsets, basis, measured):
    peers, modes = lax.axis_size("brick"), lax.axis_size("mode")
    views, slots, ray_block, voxels = weights.shape
    cap = max(2, slots // peers + 1)
    here, bins = basis.shape[1:]
    mine = bins // modes
    places_n = peers * cap
    rays = BLK_DEV * ray_block
    brick = lax.axis_index("brick")

    source, places, labels = jax.vmap(lambda o, f: slot_tables(o, f, peers, cap))(
        owners[:, :, 0], offsets
    )
    labels = jnp.moveaxis(labels.reshape(views, peers, cap), 1, 0).reshape(peers, views * cap)
    labels = jnp.pad(labels, ((0, 0), (0, 128 - views * cap))).reshape(peers, 1, 128)

    share = views * mine // peers
    view_here, bin_here = (brick * share) // mine, (brick * share) % mine
    picked = lax.dynamic_index_in_dim(basis, view_here, 0, keepdims=False)
    picked = lax.dynamic_slice_in_dim(picked.reshape(here, modes, mine), bin_here, share, 2)
    picked = picked.reshape(here, modes * share).T

    smem = pl.BlockSpec(memory_space=pltpu.SMEM)
    vmem = pl.BlockSpec(memory_space=pltpu.VMEM)
    anywhere = pl.BlockSpec(memory_space=pl.ANY)
    dma = pltpu.SemaphoreType.DMA
    chunks, width = 2 * views, mine // 2
    block = (places_n, ray_block, width)
    coeffs, residual = pl.pallas_call(
        functools.partial(kernel, peers, modes, cap),
        out_shape=(
            jax.ShapeDtypeStruct(coeffs.shape, F32),
            jax.ShapeDtypeStruct(measured.shape, F32),
        ),
        in_specs=[smem, smem, vmem, vmem] + [anywhere] * 4,
        out_specs=(anywhere, anywhere),
        scratch_shapes=[
            pltpu.VMEM(coeffs.shape, F32),
            pltpu.VMEM(coeffs.shape, BF),
            pltpu.VMEM(basis.shape, BF),
            pltpu.VMEM((views, slots * ray_block, voxels), BF),
            pltpu.VMEM((modes, views, rays // modes, mine), F32),
            pltpu.VMEM((modes, views, rays // modes, mine), F32),
            pltpu.VMEM((views, 3, 2, voxels, width), BF),
            pltpu.VMEM((chunks, 2, voxels // 2, width), BF),
            pltpu.VMEM((chunks, 2, voxels, width), BF),
            pltpu.VMEM((chunks, voxels, width), F32),
            pltpu.VMEM((chunks, voxels, width), BF),
            pltpu.VMEM((slots + 1, ray_block, width), BF),
            pltpu.VMEM((chunks,) + block, BF),
            pltpu.VMEM((chunks,) + block, BF),
            pltpu.VMEM((BLK_DEV + 1, ray_block, width), BF),
            pltpu.VMEM((chunks,) + block, BF),
            pltpu.VMEM(block, BF),
            pltpu.VMEM(block, BF),
            pltpu.VMEM(block, BF),
            pltpu.VMEM(block, BF),
            pltpu.VMEM((slots, ray_block, width), BF),
            pltpu.VMEM((width, slots * ray_block), BF),
            pltpu.VMEM((2, views, bins, voxels), BF),
            pltpu.VMEM((views, rays, places_n * ray_block), BF),
            pltpu.VMEM((views * mine, views * bins), BF),
            pltpu.VMEM((modes * share, views * bins), BF),
            pltpu.VMEM((modes - 1, share, views * bins), BF),
            pltpu.VMEM((peers, 1, 128), jnp.int32),
            pltpu.SMEM((peers, 1, 128), jnp.int32),
            pltpu.VMEM((modes, views, rays // modes, mine), F32),
            pltpu.VMEM((modes, views, rays // modes, mine), F32),
            dma((8,)),
            dma((11,)),
            dma((4,)),
            dma((4,)),
            dma((views, 4)),
            dma((views, 4)),
            dma((chunks, 6)),
            dma((chunks, 6)),
            dma((2, chunks, 6)),
            dma((2, chunks, 6)),
            dma((views, 4)),
            dma((views, 4)),
            dma((19,)),
            dma((19,)),
            dma((views, 4)),
        ],
        compiler_params=pltpu.CompilerParams(
            collective_id=0, has_side_effects=True, vmem_limit_bytes=67043328
        ),
    )(source, places, labels, picked, coeffs, weights.reshape(views, -1, voxels), basis, measured)
    return coeffs, residual


def solution(mesh):
    return jax.shard_map(
        shards,
        mesh=mesh,
        in_specs=(
            P("brick", "mode"),
            P(None, "brick", None, None),
            P(None, "brick", None),
            P(None, "brick"),
            P(None, "mode", None),
            P(None, ("brick", "mode"), None),
        ),
        out_specs=(P("brick", "mode"), P(None, ("brick", "mode"), None)),
        check_vma=False,
    )
```

```python
import functools

import jax
import jax.numpy as jnp
from jax import lax
from jax.experimental import pallas as pl
from jax.experimental.pallas import tpu as pltpu
from jax.sharding import PartitionSpec as P

BLK_DEV = 8
LEARN_RATE = 0.2
BF = jnp.bfloat16
F32 = jnp.float32
MESH = pl.DeviceIdType.MESH


def dot(a, b):
    return jnp.dot(a, b, preferred_element_type=F32)


def kernel(
    peers,
    modes,
    cap,
    owners,
    offsets,
    coeffs_hbm,
    weights_hbm,
    basis_hbm,
    measured_hbm,
    coeffs_out,
    residual_out,
    coef,
    low,
    basis,
    weight,
    chunk,
    target,
    qsend,
    qrel,
    qrecv,
    pattern,
    qlow,
    proj,
    fsend,
    frecv,
    ray,
    bsend,
    brecv0,
    brecv1,
    brecv2,
    brecv3,
    back,
    back_t,
    change,
    select,
    gram,
    gpart,
    grecv,
    label_in,
    label_s,
    result,
    collected,
    load_sem,
    local_sem,
    gs_sem,
    gr_sem,
    ts_sem,
    tr_sem,
    qs_sem,
    qr_sem,
    as_sem,
    ar_sem,
    rs_sem,
    rr_sem,
    all_s,
    all_r,
    write_sem,
    table,
    table_s,
    label_flat,
    label_out,
    column,
    mlow,
):
    brecv = (brecv0, brecv1, brecv2, brecv3)
    brick, mode = lax.axis_index("brick"), lax.axis_index("mode")
    right, left, far = [lax.rem(mode + k, modes) for k in (1, modes - 1, 2)]
    views, entries, voxels = weights_hbm.shape
    slots, ray_block = proj.shape[0] - 1, proj.shape[1]
    here, bins = basis.shape[1], basis.shape[2]
    mine = bins // modes
    places_n = peers * cap
    rays = BLK_DEV * ray_block
    tile = min(256, voxels)
    width, chunks = mine // 2, 2 * views
    half, hm = voxels // 2, width // 2
    share = gpart.shape[0] // modes

    def aligned(i, n):
        return pl.ds(pl.multiple_of(i * n, n), n)

    def to_mode(src, dst, s, r, peer):
        copy = pltpu.make_async_remote_copy(
            src_ref=src, dst_ref=dst, send_sem=s, recv_sem=r,
            device_id={"mode": peer}, device_id_type=MESH,
        )
        copy.start()

    def await_bytes(ref, sem):
        pltpu.make_async_copy(ref, ref, sem).wait()

    def to_bricks(src_of, dst, index):
        def body(k, carry):
            peer = lax.rem(brick + k, peers)
            copy = pltpu.make_async_remote_copy(
                src_ref=src_of(peer), dst_ref=dst, send_sem=all_s.at[index],
                recv_sem=all_r.at[index], device_id={"brick": peer}, device_id_type=MESH,
            )
            copy.start()
            return carry

        lax.fori_loop(1, peers, body, 0)

    loads = [
        pltpu.make_async_copy(basis_hbm, basis, load_sem.at[0]),
        pltpu.make_async_copy(coeffs_hbm, coef, load_sem.at[1]),
        pltpu.make_async_copy(weights_hbm.at[0], weight.at[0], load_sem.at[2]),
        pltpu.make_async_copy(weights_hbm.at[1], weight.at[1], load_sem.at[3]),
    ]
    loads += [
        pltpu.make_async_copy(
            measured_hbm.at[:, :, pl.ds(m * mine, mine)], chunk.at[m], load_sem.at[4 + m]
        )
        for m in range(modes)
    ]
    loads[0].start()
    loads[1].start()
    barrier = pltpu.get_barrier_semaphore()

    def greet(k, carry):
        pl.semaphore_signal(
            barrier, inc=1, device_id={"brick": lax.rem(brick + k, peers)}, device_id_type=MESH
        )
        return carry

    lax.fori_loop(1, peers, greet, 0)
    for k in range(1, modes):
        pl.semaphore_signal(
            barrier, inc=1, device_id={"mode": lax.rem(mode + k, modes)}, device_id_type=MESH
        )
    proj[slots] = jnp.zeros(proj.shape[1:], BF)
    ray[BLK_DEV] = jnp.zeros(ray.shape[1:], BF)

    def grid(rows, cols, dim):
        return lax.broadcasted_iota(jnp.int32, (rows, cols), dim)

    entry, lane = grid(slots, 128, 0), grid(slots, 128, 1)
    flat = jnp.full((peers, 128), BLK_DEV, jnp.int32)
    table[...] = jnp.zeros(table.shape, jnp.int32)
    for v in range(views):
        square = grid(slots, slots, 0) == grid(slots, slots, 1)
        owner = jnp.sum(jnp.where(square, owners[v], 0), 1, keepdims=True)
        owner_row = jnp.sum(jnp.where(entry == lane, owner, 0), 0, keepdims=True)
        earlier = (owner == owner_row) & (lane < entry)
        place = owner * cap + jnp.sum(jnp.where(earlier, 1, 0), 1, keepdims=True)
        place_row = jnp.sum(jnp.where(entry == lane, place + 1, 0), 0, keepdims=True) - 1
        offset = jnp.sum(jnp.where(square, offsets[v : v + 1, :], 0), 1, keepdims=True)
        offset_row = jnp.sum(jnp.where(entry == lane, offset, 0), 0, keepdims=True)
        source = jnp.sum(jnp.where(place == lane, entry - slots, 0), 0, keepdims=True) + slots
        table[v, 0:1, :] = source
        table[v, 1:2, :] = place_row
        for k in range(cap):
            hit = place_row == grid(peers, 128, 0) * cap + k
            label = jnp.sum(jnp.where(hit, offset_row - BLK_DEV, 0), 1, keepdims=True) + BLK_DEV
            flat = jnp.where(grid(peers, 128, 1) == v * cap + k, label, flat)
    label_flat[...] = flat

    def spread_labels(i, carry):
        label_out[i] = label_flat[pl.ds(i, 1), :]
        return carry

    lax.fori_loop(0, peers, spread_labels, 0)
    pltpu.make_async_copy(table, table_s, local_sem.at[0]).start()

    loads[0].wait()
    start = brick * share
    view_here, bin_here = start // mine, lax.rem(start, mine)
    window = bin_here // 128
    picked = []
    for m in range(modes):
        lanes = pl.ds(pl.multiple_of(m * mine + window * 128, 128), 128)
        column[m] = basis[view_here, :, lanes].astype(F32).T.astype(BF)
        rows = pl.ds(pl.multiple_of(lax.rem(bin_here, 128), share), share)
        picked.append(column[m, rows, :])
    picked = jnp.concatenate(picked, 0)
    def half_basis(u, h):
        return jnp.concatenate(
            [basis[u, :, m * mine + h * width : m * mine + (h + 1) * width] for m in range(modes)], 1
        )

    for u in range(views):
        for h in range(2):
            at = u * bins + h * bins // 2
            gpart[:, at : at + bins // 2] = dot(picked, half_basis(u, h)).astype(BF)
    loads[1].wait()
    for load in loads[2:]:
        load.start()
    pltpu.make_async_copy(table, table_s, local_sem.at[0]).wait()

    def round_low(i, carry):
        low[aligned(i, tile), :] = coef[aligned(i, tile), :].astype(BF)
        return carry

    lax.fori_loop(0, voxels // tile, round_low, 0)

    lower, upper = pl.ds(0, half), pl.ds(half, half)

    def partial_patterns(v):
        def body(i, carry):
            rows = aligned(i, tile)
            for slot, m in ((0, far), (1, right), (2, left)):
                value = dot(low[rows, :], basis[v, :, aligned(m, mine)]).astype(BF)
                for h in range(2):
                    qsend[v, slot, h, rows, :] = value[:, h * width : (h + 1) * width]
            return carry

        lax.fori_loop(0, voxels // tile, body, 0)

    def own_pattern(v):
        def body(i, carry):
            rows = aligned(i, tile)
            value = dot(low[rows, :], basis[v, :, aligned(mode, mine)])
            for h in range(2):
                pattern[2 * v + h, rows, :] = value[:, h * width : (h + 1) * width]
            return carry

        lax.fori_loop(0, voxels // tile, body, 0)

    def scatter_send(c):
        v, h = c // 2, c % 2
        for k, (slot, part, dst, peer) in enumerate(
            (
                (0, upper, qrel.at[c, 0], right),
                (0, lower, qrel.at[c, 1], left),
                (1, lower, qrecv.at[c, 0, lower], right),
                (2, upper, qrecv.at[c, 1, upper], left),
            )
        ):
            to_mode(qsend.at[v, slot, h, part], dst, qs_sem.at[c, k], qr_sem.at[c, k], peer)

    def scatter_relay(c):
        v, h = c // 2, c % 2
        for k, (slot, start, part, peer) in enumerate(((1, half, upper, right), (2, 0, lower, left))):
            await_bytes(qrel.at[c, k], qr_sem.at[c, k])

            def body(i, carry, k=k, slot=slot, start=start):
                rows = pl.ds(pl.multiple_of(start + i * (tile // 2), tile // 2), tile // 2)
                given = qrel[c, k, aligned(i, tile // 2), :].astype(F32)
                total = qsend[v, slot, h, rows, :].astype(F32) + given
                qsend[v, slot, h, rows, :] = total.astype(BF)
                return carry

            lax.fori_loop(0, half // (tile // 2), body, 0)
            to_mode(
                qsend.at[v, slot, h, part], qrecv.at[c, k, part],
                qs_sem.at[c, 4 + k], qr_sem.at[c, 4 + k], peer,
            )

    def scatter_end(c):
        for k, part in ((2, lower), (3, upper), (4, upper), (5, lower)):
            await_bytes(qrecv.at[c, 0, part], qr_sem.at[c, k])

        def body(i, carry):
            rows = aligned(i, tile)
            total = pattern[c, rows, :] + qrecv[c, 0, rows, :].astype(F32)
            total = total + qrecv[c, 1, rows, :].astype(F32)
            pattern[c, rows, :] = total
            qlow[c, rows, :] = total.astype(BF)
            return carry

        lax.fori_loop(0, voxels // tile, body, 0)

    def share_gram():
        own = aligned(mode, share)
        for k in range(1, modes):
            await_bytes(grecv.at[k - 1], gr_sem.at[k])
        total = gpart[own, :].astype(F32)
        for k in range(1, modes):
            total = total + grecv[k - 1].astype(F32)
        gram[aligned(brick, share), :] = total.astype(BF)
        rows = gram.at[aligned(brick, share)]

        def body(k, carry):
            peer = lax.rem(brick + 2 * k, peers)
            copy = pltpu.make_async_remote_copy(
                src_ref=rows, dst_ref=rows, send_sem=all_s.at[1],
                recv_sem=all_r.at[1], device_id={"brick": peer}, device_id_type=MESH,
            )
            copy.start()
            return carry

        lax.fori_loop(1, peers // 2, body, 0)

    def hand_gram():
        await_bytes(gram.at[pl.ds(0, (peers // 2 - 1) * share)], all_r.at[1])
        core = lax.rem(brick, 2)
        twin = brick + 1 - 2 * core

        def body(k, carry):
            rows = gram.at[aligned(2 * k + core, share)]
            copy = pltpu.make_async_remote_copy(
                src_ref=rows, dst_ref=rows, send_sem=all_s.at[2],
                recv_sem=all_r.at[2], device_id={"brick": twin}, device_id_type=MESH,
            )
            copy.start()
            return carry

        lax.fori_loop(0, peers // 2, body, 0)

    def share_measured(v):
        for k in range(1, modes):
            peer = lax.rem(mode + k, modes)
            to_mode(
                mlow.at[peer, v], target.at[mode, v], ts_sem.at[v, k], tr_sem.at[v, k], peer
            )
        pltpu.make_async_copy(mlow.at[mode, v], target.at[mode, v], local_sem.at[1 + v]).start()

    def measured_end(v):
        for k in range(1, modes):
            await_bytes(target.at[0, v], tr_sem.at[v, k])
        pltpu.make_async_copy(mlow.at[mode, v], target.at[mode, v], local_sem.at[1 + v]).wait()

    def share_result(v):
        for k in range(1, modes):
            peer = lax.rem(mode + k, modes)
            to_mode(
                result.at[peer, v], collected.at[mode, v], rs_sem.at[v, k], rr_sem.at[v, k], peer
            )
        pltpu.make_async_copy(
            result.at[mode, v], collected.at[mode, v], local_sem.at[1 + v]
        ).start()

    def result_end(v):
        for k in range(1, modes):
            await_bytes(collected.at[0, v], rr_sem.at[v, k])
        pltpu.make_async_copy(
            result.at[mode, v], collected.at[mode, v], local_sem.at[1 + v]
        ).wait()

    group = 128 // ray_block

    def build_select():
        await_bytes(label_in.at[pl.ds(0, peers - 1)], all_r.at[0])
        pltpu.make_async_copy(label_out.at[brick], label_in.at[brick], local_sem.at[0]).wait()
        lookup = pltpu.make_async_copy(label_in, label_s, local_sem.at[0])
        lookup.start()
        lookup.wait()

        def build(t, carry):
            row = lax.broadcasted_iota(jnp.int32, (rays, 128), 0)
            lane = lax.broadcasted_iota(jnp.int32, (rays, 128), 1)
            for v in range(views):
                want = jnp.zeros((rays, 128), jnp.int32)
                for g in range(group):
                    entry = t * group + g
                    label = label_s[entry // cap, 0, v * cap + entry % cap]
                    inside = (lane >= g * ray_block) & (lane < (g + 1) * ray_block)
                    want = jnp.where(inside, label * ray_block + lane - g * ray_block, want)
                select[v, :, aligned(t, 128)] = jnp.where(want == row, 1.0, 0.0).astype(BF)
            return carry

        lax.fori_loop(0, places_n // group, build, 0)

    own_slots = pl.ds(brick * cap, cap)
    others = pl.ds(0, places_n - cap)

    def forward(s, c):
        v = c // 2

        def body(i, carry):
            value = dot(weight[v, aligned(i, rays), :], qlow[c]).astype(BF)
            proj[pl.ds(i * BLK_DEV, BLK_DEV)] = value.reshape(BLK_DEV, ray_block, width)
            return carry

        lax.fori_loop(0, entries // rays, body, 0)
        if s:
            await_bytes(fsend.at[c, others], all_s.at[3 + c])

        def pack(i, carry):
            fsend[c, i] = proj[table_s[v, 0, i]]
            return carry

        lax.fori_loop(0, places_n, pack, 0, unroll=8)
        to_bricks(
            lambda peer: fsend.at[c, pl.ds(peer * cap, cap)], frecv.at[c, own_slots], 3 + 4 * s + c
        )
        pltpu.make_async_copy(
            fsend.at[c, own_slots], frecv.at[c, own_slots], local_sem.at[3 + c]
        ).start()

    def reflect(s, c):
        v, h = c // 2, c % 2
        lanes = slice(h * width, (h + 1) * width)
        await_bytes(frecv.at[c, others], all_r.at[3 + 4 * s + c])
        pltpu.make_async_copy(
            fsend.at[c, own_slots], frecv.at[c, own_slots], local_sem.at[3 + c]
        ).wait()
        goal = jnp.concatenate([target[m, v, :, lanes] for m in range(modes)], 0)
        value = dot(select[v], frecv[c].reshape(places_n * ray_block, width))
        if s:
            result[:, v, :, lanes] = value.reshape(modes, rays // modes, width)
            await_bytes(bsend.at[c, others], all_s.at[11 + c])
        value = value - goal.astype(F32)
        ray[pl.ds(0, BLK_DEV)] = value.astype(BF).reshape(BLK_DEV, ray_block, width)

        def answer(p, carry):
            for k in range(cap):
                bsend[c, p * cap + k] = ray[label_s[p, 0, v * cap + k]]
            return carry

        lax.fori_loop(0, peers, answer, 0, unroll=4)
        to_bricks(
            lambda peer: bsend.at[c, pl.ds(peer * cap, cap)], brecv[c].at[own_slots], 11 + 4 * s + c
        )
        pltpu.make_async_copy(
            bsend.at[c, own_slots], brecv[c].at[own_slots], local_sem.at[7 + c]
        ).start()

    def adjoint(s, c):
        v, h = c // 2, c % 2
        await_bytes(brecv[c].at[others], all_r.at[11 + 4 * s + c])
        pltpu.make_async_copy(
            bsend.at[c, own_slots], brecv[c].at[own_slots], local_sem.at[7 + c]
        ).wait()

        def unpack(i, carry):
            back[i] = brecv[c][table_s[v, 1, i]]
            return carry

        lax.fori_loop(0, slots, unpack, 0, unroll=8)

        def turn(i, carry):
            piece = back[pl.ds(i * BLK_DEV, BLK_DEV)].reshape(rays, width).astype(F32)
            back_t[:, aligned(i, rays)] = piece.T.astype(BF)
            return carry

        lax.fori_loop(0, entries // rays, turn, 0)
        rows = aligned(h * modes + mode, width)

        def body(j, carry):
            cols = aligned(j, tile)
            change[s, v, rows, cols] = dot(back_t[...], weight[v, :, cols]).astype(BF)
            return carry

        lax.fori_loop(0, voxels // tile, body, 0)
        for k, (skip, peer) in enumerate(((hm, right), (0, right), (0, left), (hm, left))):
            part = change.at[
                s, v, pl.ds(pl.multiple_of((h * modes + mode) * width + skip, hm), hm)
            ]
            to_mode(part, part, as_sem.at[s, c, k], ar_sem.at[s, c, k], peer)

    def gather_relay(s, c):
        v, h = c // 2, c % 2
        for k, (giver, skip, peer) in enumerate(((left, hm, right), (right, 0, left))):
            part = change.at[
                s, v, pl.ds(pl.multiple_of((h * modes + giver) * width + skip, hm), hm)
            ]
            await_bytes(part, ar_sem.at[s, c, 2 * k])
            to_mode(part, part, as_sem.at[s, c, 4 + k], ar_sem.at[s, c, 4 + k], peer)

    def gather_end(s, c):
        for k in (1, 3, 4, 5):
            await_bytes(change.at[s, c // 2, pl.ds(0, hm)], ar_sem.at[s, c, k])

    def renew(c, low_chunk, high_chunk):
        u, h = c // 2, c % 2
        part = pl.ds(h * bins // 2, bins // 2)
        at = u * bins + h * bins // 2
        rows = slice(low_chunk * width, high_chunk * width)

        def body(j, carry):
            cols = aligned(j, tile)
            step = dot(gram[rows, at : at + bins // 2], change[0, u, part, cols]).T
            for d in range(low_chunk, high_chunk):
                i = d - low_chunk
                value = pattern[d, cols, :] - LEARN_RATE * step[:, i * width : (i + 1) * width]
                pattern[d, cols, :] = value
                if c == chunks - 1:
                    qlow[d, cols, :] = value.astype(BF)
            return carry

        lax.fori_loop(0, voxels // tile, body, 0)

    def update(s, u, halves, out=False):
        def body(j, carry):
            cols = aligned(j, tile)
            if len(halves) == 2:
                lhs = jnp.concatenate([half_basis(u, h) for h in range(2)], 1)
                step = dot(lhs, change[s, u, :, cols]).T
            else:
                part = pl.ds(halves[0] * bins // 2, bins // 2)
                step = dot(half_basis(u, halves[0]), change[s, u, part, cols]).T
            coef[cols, :] = coef[cols, :] - LEARN_RATE * step
            if out:
                pltpu.make_async_copy(
                    coef.at[cols], coeffs_out.at[cols], load_sem.at[j]
                ).start()
            return carry

        lax.fori_loop(0, voxels // tile, body, 0)

    partial_patterns(0)
    pl.semaphore_wait(barrier, peers - 1 + modes - 1)

    for k in range(1, modes):
        peer = lax.rem(mode + k, modes)
        to_mode(gpart.at[aligned(peer, share)], grecv.at[k - 1], gs_sem.at[k], gr_sem.at[k], peer)
    to_bricks(lambda peer: label_out.at[peer], label_in.at[brick], 0)
    pltpu.make_async_copy(label_out.at[brick], label_in.at[brick], local_sem.at[0]).start()
    scatter_send(0)
    own_pattern(0)
    partial_patterns(1)
    own_pattern(1)
    share_gram()
    for m in range(modes):
        loads[4 + m].wait()
    mlow[...] = chunk[...].astype(BF)
    scatter_relay(0)
    share_measured(0)
    scatter_send(1)
    build_select()
    loads[2].wait()
    scatter_end(0)
    forward(0, 0)
    scatter_relay(1)
    scatter_send(2)
    measured_end(0)
    reflect(0, 0)
    scatter_end(1)
    forward(0, 1)
    scatter_relay(2)
    share_measured(1)
    scatter_send(3)
    loads[3].wait()
    scatter_end(2)
    forward(0, 2)
    scatter_relay(3)
    adjoint(0, 0)
    reflect(0, 1)
    scatter_end(3)
    forward(0, 3)
    gather_relay(0, 0)
    measured_end(1)
    reflect(0, 2)
    hand_gram()
    adjoint(0, 1)
    reflect(0, 3)
    gather_relay(0, 1)
    adjoint(0, 2)
    gather_end(0, 0)
    await_bytes(gram.at[pl.ds(0, peers // 2 * share)], all_r.at[2])
    renew(0, 0, chunks)
    gather_end(0, 1)
    renew(1, 0, chunks)
    gather_relay(0, 2)
    adjoint(0, 3)
    gather_relay(0, 3)
    gather_end(0, 2)
    renew(2, 0, chunks)
    gather_end(0, 3)
    renew(3, 0, 1)
    forward(1, 0)
    renew(3, 1, chunks)
    forward(1, 1)
    update(0, 0, (0, 1))
    reflect(1, 0)
    forward(1, 2)
    reflect(1, 1)
    forward(1, 3)
    share_result(0)
    update(0, 1, (0,))
    adjoint(1, 0)
    reflect(1, 2)
    gather_relay(1, 0)
    update(0, 1, (1,))
    adjoint(1, 1)
    reflect(1, 3)
    gather_relay(1, 1)
    adjoint(1, 2)
    gather_relay(1, 2)
    adjoint(1, 3)
    gather_end(1, 0)
    gather_end(1, 1)
    update(1, 0, (0, 1))
    gather_relay(1, 3)
    share_result(1)
    writes = []

    def write_residual(v):
        result_end(v)
        collected[:, v] = collected[:, v] - chunk[:, v]
        for m in range(modes):
            write = pltpu.make_async_copy(
                collected.at[m, v],
                residual_out.at[v, :, pl.ds(m * mine, mine)],
                write_sem.at[v, m],
            )
            write.start()
            writes.append(write)

    write_residual(0)
    gather_end(1, 2)
    update(1, 1, (0,))
    gather_end(1, 3)
    update(1, 1, (1,), True)
    write_residual(1)

    for k in range(1, modes):
        await_bytes(grecv.at[0], gs_sem.at[k])
        for v in range(views):
            await_bytes(mlow.at[0, v], ts_sem.at[v, k])
            await_bytes(result.at[0, v], rs_sem.at[v, k])
    for c in range(2 * views):
        for k in range(6):
            await_bytes(qrel.at[0, 0], qs_sem.at[c, k])
            for s in range(2):
                await_bytes(change.at[0, 0, pl.ds(0, hm)], as_sem.at[s, c, k])
        await_bytes(fsend.at[c, others], all_s.at[7 + c])
        await_bytes(bsend.at[c, others], all_s.at[15 + c])
    await_bytes(label_in.at[pl.ds(0, peers - 1)], all_s.at[0])
    await_bytes(gram.at[pl.ds(0, (peers // 2 - 1) * share)], all_s.at[1])
    await_bytes(gram.at[pl.ds(0, peers // 2 * share)], all_s.at[2])
    for write in writes:
        write.wait()

    def drain(j, carry):
        cols = aligned(j, tile)
        pltpu.make_async_copy(coef.at[cols], coeffs_out.at[cols], load_sem.at[j]).wait()
        return carry

    lax.fori_loop(0, voxels // tile, drain, 0)


def shards(coeffs, weights, owners, offsets, basis, measured):
    peers, modes = lax.axis_size("brick"), lax.axis_size("mode")
    views, slots, ray_block, voxels = weights.shape
    cap = max(2, slots // peers + 1)
    here, bins = basis.shape[1:]
    mine = bins // modes
    places_n = peers * cap
    rays = BLK_DEV * ray_block
    share = views * mine // peers

    vmem = pl.BlockSpec(memory_space=pltpu.VMEM)
    anywhere = pl.BlockSpec(memory_space=pl.ANY)
    dma = pltpu.SemaphoreType.DMA
    chunks, width = 2 * views, mine // 2
    block = (places_n, ray_block, width)
    coeffs, residual = pl.pallas_call(
        functools.partial(kernel, peers, modes, cap),
        out_shape=(
            jax.ShapeDtypeStruct(coeffs.shape, F32),
            jax.ShapeDtypeStruct(measured.shape, F32),
        ),
        in_specs=[vmem, vmem] + [anywhere] * 4,
        out_specs=(anywhere, anywhere),
        scratch_shapes=[
            pltpu.VMEM(coeffs.shape, F32),
            pltpu.VMEM(coeffs.shape, BF),
            pltpu.VMEM(basis.shape, BF),
            pltpu.VMEM((views, slots * ray_block, voxels), BF),
            pltpu.VMEM((modes, views, rays // modes, mine), F32),
            pltpu.VMEM((modes, views, rays // modes, mine), BF),
            pltpu.VMEM((views, 3, 2, voxels, width), BF),
            pltpu.VMEM((chunks, 2, voxels // 2, width), BF),
            pltpu.VMEM((chunks, 2, voxels, width), BF),
            pltpu.VMEM((chunks, voxels, width), F32),
            pltpu.VMEM((chunks, voxels, width), BF),
            pltpu.VMEM((slots + 1, ray_block, width), BF),
            pltpu.VMEM((chunks,) + block, BF),
            pltpu.VMEM((chunks,) + block, BF),
            pltpu.VMEM((BLK_DEV + 1, ray_block, width), BF),
            pltpu.VMEM((chunks,) + block, BF),
            pltpu.VMEM(block, BF),
            pltpu.VMEM(block, BF),
            pltpu.VMEM(block, BF),
            pltpu.VMEM(block, BF),
            pltpu.VMEM((slots, ray_block, width), BF),
            pltpu.VMEM((width, slots * ray_block), BF),
            pltpu.VMEM((2, views, bins, voxels), BF),
            pltpu.VMEM((views, rays, places_n * ray_block), BF),
            pltpu.VMEM((views * mine, views * bins), BF),
            pltpu.VMEM((modes * share, views * bins), BF),
            pltpu.VMEM((modes - 1, share, views * bins), BF),
            pltpu.VMEM((peers, 1, 128), jnp.int32),
            pltpu.SMEM((peers, 1, 128), jnp.int32),
            pltpu.VMEM((modes, views, rays // modes, mine), F32),
            pltpu.VMEM((modes, views, rays // modes, mine), F32),
            dma((8,)),
            dma((11,)),
            dma((4,)),
            dma((4,)),
            dma((views, 4)),
            dma((views, 4)),
            dma((chunks, 6)),
            dma((chunks, 6)),
            dma((2, chunks, 6)),
            dma((2, chunks, 6)),
            dma((views, 4)),
            dma((views, 4)),
            dma((19,)),
            dma((19,)),
            dma((views, 4)),
            pltpu.VMEM((views, 8, 128), jnp.int32),
            pltpu.SMEM((views, 8, 128), jnp.int32),
            pltpu.VMEM((peers, 128), jnp.int32),
            pltpu.VMEM((peers, 1, 128), jnp.int32),
            pltpu.VMEM((modes, 128, here), BF),
            pltpu.VMEM((modes, views, rays // modes, mine), BF),
        ],
        compiler_params=pltpu.CompilerParams(
            collective_id=0, has_side_effects=True, vmem_limit_bytes=67043328
        ),
    )(owners.reshape(views, 1, slots), offsets, coeffs, weights.reshape(views, -1, voxels), basis, measured)
    return coeffs, residual


def solution(mesh):
    return jax.shard_map(
        shards,
        mesh=mesh,
        in_specs=(
            P("brick", "mode"),
            P(None, "brick", None, None),
            P(None, "brick", None),
            P(None, "brick"),
            P(None, "mode", None),
            P(None, ("brick", "mode"), None),
        ),
        out_specs=(P("brick", "mode"), P(None, ("brick", "mode"), None)),
        check_vma=False,
    )
```

```python
import functools
import math

import jax
import jax.numpy as jnp
from jax import lax
from jax.experimental import pallas as pl
from jax.experimental.pallas import tpu as pltpu
from jax.sharding import PartitionSpec as P

BLK_DEV = 8
LEARN_RATE = 0.2
BF = jnp.bfloat16
F32 = jnp.float32
MESH = pl.DeviceIdType.MESH


def dot(a, b):
    return jnp.dot(a, b, preferred_element_type=F32)


def hand_over(coeffs, residual, coeffs_out, residual_out, rows, rays, in_sem, out_sem):
    pieces = in_sem.shape[0] - 1
    part = coeffs.shape[0] // pieces
    moves = [(coeffs, rows, coeffs_out, pl.ds(i * part, part)) for i in range(pieces)]
    moves.append((residual, rays, residual_out, pl.ds(0, residual.shape[0])))
    ins = [
        pltpu.make_async_copy(src.at[at], mid.at[at], in_sem.at[i])
        for i, (src, mid, dst, at) in enumerate(moves)
    ]
    outs = [
        pltpu.make_async_copy(mid.at[at], dst.at[at], out_sem.at[i])
        for i, (src, mid, dst, at) in enumerate(moves)
    ]
    for move in ins:
        move.start()
    for first, second in zip(ins, outs):
        first.wait()
        second.start()
    for move in outs:
        move.wait()


def kernel(
    peers,
    modes,
    cap,
    owners,
    offsets,
    coeffs_hbm,
    weights_hbm,
    basis_hbm,
    measured_hbm,
    coeffs_out,
    residual_out,
    coef,
    low,
    basis,
    weight,
    chunk,
    target,
    qsend,
    qrel,
    qrecv,
    pattern,
    qlow,
    proj,
    fsend,
    frecv,
    ray,
    bsend,
    brecv0,
    brecv1,
    brecv2,
    brecv3,
    back,
    back_t,
    change,
    select,
    gram,
    gpart,
    grecv,
    label_in,
    label_s,
    result,
    collected,
    load_sem,
    local_sem,
    gs_sem,
    gr_sem,
    ts_sem,
    tr_sem,
    qs_sem,
    qr_sem,
    as_sem,
    ar_sem,
    rs_sem,
    rr_sem,
    all_s,
    all_r,
    write_sem,
    table,
    table_s,
    label_flat,
    label_out,
    column,
    mlow,
):
    brecv = (brecv0, brecv1, brecv2, brecv3)
    brick, mode = lax.axis_index("brick"), lax.axis_index("mode")
    right, left, far = [lax.rem(mode + k, modes) for k in (1, modes - 1, 2)]
    views, entries, voxels = weights_hbm.shape
    slots, ray_block = proj.shape[0] - 1, proj.shape[1]
    here, bins = basis.shape[1], basis.shape[2]
    mine = bins // modes
    places_n = peers * cap
    rays = BLK_DEV * ray_block
    tile = min(256, voxels)
    width, chunks = mine // 2, 2 * views
    half, hm = voxels // 2, width // 2
    share = gpart.shape[0] // modes

    def aligned(i, n):
        return pl.ds(pl.multiple_of(i * n, n), n)

    def to_mode(src, dst, s, r, peer):
        copy = pltpu.make_async_remote_copy(
            src_ref=src, dst_ref=dst, send_sem=s, recv_sem=r,
            device_id={"mode": peer}, device_id_type=MESH,
        )
        copy.start()

    def await_bytes(ref, sem):
        pltpu.make_async_copy(ref, ref, sem).wait()

    side = math.isqrt(peers // 2)
    deep = peers // (2 * side)

    def partner(dz, dy, dc):
        z = lax.rem(brick // (2 * side) + dz, deep)
        y = lax.rem(lax.rem(brick // 2, side) + dy, side)
        return (z * side + y) * 2 + lax.rem(lax.rem(brick, 2) + dc, 2)

    def to_bricks(src_of, dst, index):
        def body(k, carry):
            q = lax.rem(k * 13, peers)
            peer = partner(q // (2 * side), lax.rem(q // 2, side), lax.rem(q, 2))
            copy = pltpu.make_async_remote_copy(
                src_ref=src_of(peer), dst_ref=dst, send_sem=all_s.at[index],
                recv_sem=all_r.at[index], device_id={"brick": peer}, device_id_type=MESH,
            )
            copy.start()
            return carry

        lax.fori_loop(1, peers, body, 0)

    loads = [
        pltpu.make_async_copy(basis_hbm, basis, load_sem.at[0]),
        pltpu.make_async_copy(coeffs_hbm, coef, load_sem.at[1]),
        pltpu.make_async_copy(weights_hbm.at[0], weight.at[0], load_sem.at[2]),
        pltpu.make_async_copy(weights_hbm.at[1], weight.at[1], load_sem.at[3]),
    ]
    loads += [
        pltpu.make_async_copy(
            measured_hbm.at[:, :, pl.ds(m * mine, mine)], chunk.at[m], load_sem.at[4 + m]
        )
        for m in range(modes)
    ]
    loads[0].start()
    loads[1].start()
    barrier = pltpu.get_barrier_semaphore()

    def greet(k, carry):
        pl.semaphore_signal(
            barrier, inc=1, device_id={"brick": lax.rem(brick + k, peers)}, device_id_type=MESH
        )
        return carry

    lax.fori_loop(1, peers, greet, 0)
    for k in range(1, modes):
        pl.semaphore_signal(
            barrier, inc=1, device_id={"mode": lax.rem(mode + k, modes)}, device_id_type=MESH
        )
    proj[slots] = jnp.zeros(proj.shape[1:], BF)
    ray[BLK_DEV] = jnp.zeros(ray.shape[1:], BF)

    def grid(rows, cols, dim):
        return lax.broadcasted_iota(jnp.int32, (rows, cols), dim)

    entry, lane = grid(slots, 128, 0), grid(slots, 128, 1)
    flat = jnp.full((peers, 128), BLK_DEV, jnp.int32)
    table[...] = jnp.zeros(table.shape, jnp.int32)
    for v in range(views):
        square = grid(slots, slots, 0) == grid(slots, slots, 1)
        owner = jnp.sum(jnp.where(square, owners[v], 0), 1, keepdims=True)
        owner_row = jnp.sum(jnp.where(entry == lane, owner, 0), 0, keepdims=True)
        earlier = (owner == owner_row) & (lane < entry)
        place = owner * cap + jnp.sum(jnp.where(earlier, 1, 0), 1, keepdims=True)
        place_row = jnp.sum(jnp.where(entry == lane, place + 1, 0), 0, keepdims=True) - 1
        offset = jnp.sum(jnp.where(square, offsets[v : v + 1, :], 0), 1, keepdims=True)
        offset_row = jnp.sum(jnp.where(entry == lane, offset, 0), 0, keepdims=True)
        source = jnp.sum(jnp.where(place == lane, entry - slots, 0), 0, keepdims=True) + slots
        table[v, 0:1, :] = source
        table[v, 1:2, :] = place_row
        for k in range(cap):
            hit = place_row == grid(peers, 128, 0) * cap + k
            label = jnp.sum(jnp.where(hit, offset_row - BLK_DEV, 0), 1, keepdims=True) + BLK_DEV
            flat = jnp.where(grid(peers, 128, 1) == v * cap + k, label, flat)
    label_flat[...] = flat

    def spread_labels(i, carry):
        label_out[i] = label_flat[pl.ds(i, 1), :]
        return carry

    lax.fori_loop(0, peers, spread_labels, 0)
    pltpu.make_async_copy(table, table_s, local_sem.at[0]).start()

    loads[0].wait()
    start = brick * share
    view_here, bin_here = start // mine, lax.rem(start, mine)
    window = bin_here // 128
    picked = []
    for m in range(modes):
        lanes = pl.ds(pl.multiple_of(m * mine + window * 128, 128), 128)
        column[m] = basis[view_here, :, lanes].astype(F32).T.astype(BF)
        rows = pl.ds(pl.multiple_of(lax.rem(bin_here, 128), share), share)
        picked.append(column[m, rows, :])
    picked = jnp.concatenate(picked, 0)
    def half_basis(u, h):
        return jnp.concatenate(
            [basis[u, :, m * mine + h * width : m * mine + (h + 1) * width] for m in range(modes)], 1
        )

    for u in range(views):
        for h in range(2):
            at = u * bins + h * bins // 2
            gpart[:, at : at + bins // 2] = dot(picked, half_basis(u, h)).astype(BF)
    loads[1].wait()
    for load in loads[2:]:
        load.start()
    pltpu.make_async_copy(table, table_s, local_sem.at[0]).wait()

    def round_low(i, carry):
        low[aligned(i, tile), :] = coef[aligned(i, tile), :].astype(BF)
        return carry

    lax.fori_loop(0, voxels // tile, round_low, 0)

    lower, upper = pl.ds(0, half), pl.ds(half, half)

    def partial_patterns(v):
        def body(i, carry):
            rows = aligned(i, tile)
            for slot, m in ((0, far), (1, right), (2, left)):
                value = dot(low[rows, :], basis[v, :, aligned(m, mine)]).astype(BF)
                for h in range(2):
                    qsend[v, slot, h, rows, :] = value[:, h * width : (h + 1) * width]
            return carry

        lax.fori_loop(0, voxels // tile, body, 0)

    def own_pattern(v):
        def body(i, carry):
            rows = aligned(i, tile)
            value = dot(low[rows, :], basis[v, :, aligned(mode, mine)])
            for h in range(2):
                pattern[2 * v + h, rows, :] = value[:, h * width : (h + 1) * width]
            return carry

        lax.fori_loop(0, voxels // tile, body, 0)

    def scatter_send(c):
        v, h = c // 2, c % 2
        for k, (slot, part, dst, peer) in enumerate(
            (
                (0, upper, qrel.at[c, 0], right),
                (0, lower, qrel.at[c, 1], left),
                (1, lower, qrecv.at[c, 0, lower], right),
                (2, upper, qrecv.at[c, 1, upper], left),
            )
        ):
            to_mode(qsend.at[v, slot, h, part], dst, qs_sem.at[c, k], qr_sem.at[c, k], peer)

    def scatter_relay(c):
        v, h = c // 2, c % 2
        for k, (slot, start, part, peer) in enumerate(((1, half, upper, right), (2, 0, lower, left))):
            await_bytes(qrel.at[c, k], qr_sem.at[c, k])

            def body(i, carry, k=k, slot=slot, start=start):
                rows = pl.ds(pl.multiple_of(start + i * (tile // 2), tile // 2), tile // 2)
                given = qrel[c, k, aligned(i, tile // 2), :].astype(F32)
                total = qsend[v, slot, h, rows, :].astype(F32) + given
                qsend[v, slot, h, rows, :] = total.astype(BF)
                return carry

            lax.fori_loop(0, half // (tile // 2), body, 0)
            to_mode(
                qsend.at[v, slot, h, part], qrecv.at[c, k, part],
                qs_sem.at[c, 4 + k], qr_sem.at[c, 4 + k], peer,
            )

    def scatter_end(c):
        for k, part in ((2, lower), (3, upper), (4, upper), (5, lower)):
            await_bytes(qrecv.at[c, 0, part], qr_sem.at[c, k])

        def body(i, carry):
            rows = aligned(i, tile)
            total = pattern[c, rows, :] + qrecv[c, 0, rows, :].astype(F32)
            total = total + qrecv[c, 1, rows, :].astype(F32)
            pattern[c, rows, :] = total
            qlow[c, rows, :] = total.astype(BF)
            return carry

        lax.fori_loop(0, voxels // tile, body, 0)

    def share_gram():
        own = aligned(mode, share)
        for k in range(1, modes):
            await_bytes(grecv.at[k - 1], gr_sem.at[k])
        total = gpart[own, :].astype(F32)
        for k in range(1, modes):
            total = total + grecv[k - 1].astype(F32)
        gram[aligned(brick, share), :] = total.astype(BF)
        rows = gram.at[aligned(brick, share)]

        def body(k, carry):
            q = lax.rem(k * 5, peers // 2)
            peer = partner(q // side, lax.rem(q, side), 0)
            copy = pltpu.make_async_remote_copy(
                src_ref=rows, dst_ref=rows, send_sem=all_s.at[1],
                recv_sem=all_r.at[1], device_id={"brick": peer}, device_id_type=MESH,
            )
            copy.start()
            return carry

        lax.fori_loop(1, peers // 2, body, 0)

    def hand_gram():
        await_bytes(gram.at[pl.ds(0, (peers // 2 - 1) * share)], all_r.at[1])
        core = lax.rem(brick, 2)
        twin = brick + 1 - 2 * core

        def body(k, carry):
            rows = gram.at[aligned(2 * k + core, share)]
            copy = pltpu.make_async_remote_copy(
                src_ref=rows, dst_ref=rows, send_sem=all_s.at[2],
                recv_sem=all_r.at[2], device_id={"brick": twin}, device_id_type=MESH,
            )
            copy.start()
            return carry

        lax.fori_loop(0, peers // 2, body, 0)

    def share_measured(v):
        for k in range(1, modes):
            peer = lax.rem(mode + k, modes)
            to_mode(
                mlow.at[peer, v], target.at[mode, v], ts_sem.at[v, k], tr_sem.at[v, k], peer
            )
        pltpu.make_async_copy(mlow.at[mode, v], target.at[mode, v], local_sem.at[1 + v]).start()

    def measured_end(v):
        for k in range(1, modes):
            await_bytes(target.at[0, v], tr_sem.at[v, k])
        pltpu.make_async_copy(mlow.at[mode, v], target.at[mode, v], local_sem.at[1 + v]).wait()

    def share_result(v):
        for k in range(1, modes):
            peer = lax.rem(mode + k, modes)
            to_mode(
                result.at[peer, v], collected.at[mode, v], rs_sem.at[v, k], rr_sem.at[v, k], peer
            )
        pltpu.make_async_copy(
            result.at[mode, v], collected.at[mode, v], local_sem.at[1 + v]
        ).start()

    def result_end(v):
        for k in range(1, modes):
            await_bytes(collected.at[0, v], rr_sem.at[v, k])
        pltpu.make_async_copy(
            result.at[mode, v], collected.at[mode, v], local_sem.at[1 + v]
        ).wait()

    group = 128 // ray_block

    def build_select():
        await_bytes(label_in.at[pl.ds(0, peers - 1)], all_r.at[0])
        pltpu.make_async_copy(label_out.at[brick], label_in.at[brick], local_sem.at[0]).wait()
        lookup = pltpu.make_async_copy(label_in, label_s, local_sem.at[0])
        lookup.start()
        lookup.wait()

        def build(t, carry):
            row = lax.broadcasted_iota(jnp.int32, (rays, 128), 0)
            lane = lax.broadcasted_iota(jnp.int32, (rays, 128), 1)
            for v in range(views):
                want = jnp.zeros((rays, 128), jnp.int32)
                for g in range(group):
                    entry = t * group + g
                    label = label_s[entry // cap, 0, v * cap + entry % cap]
                    inside = (lane >= g * ray_block) & (lane < (g + 1) * ray_block)
                    want = jnp.where(inside, label * ray_block + lane - g * ray_block, want)
                select[v, :, aligned(t, 128)] = jnp.where(want == row, 1.0, 0.0).astype(BF)
            return carry

        lax.fori_loop(0, places_n // group, build, 0)

    own_slots = pl.ds(brick * cap, cap)
    others = pl.ds(0, places_n - cap)

    def forward(s, c):
        v = c // 2

        def body(i, carry):
            value = dot(weight[v, aligned(i, rays), :], qlow[c]).astype(BF)
            proj[pl.ds(i * BLK_DEV, BLK_DEV)] = value.reshape(BLK_DEV, ray_block, width)
            return carry

        lax.fori_loop(0, entries // rays, body, 0)
        if s:
            await_bytes(fsend.at[c, others], all_s.at[3 + c])

        def pack(i, carry):
            fsend[c, i] = proj[table_s[v, 0, i]]
            return carry

        lax.fori_loop(0, places_n, pack, 0, unroll=8)
        to_bricks(
            lambda peer: fsend.at[c, pl.ds(peer * cap, cap)], frecv.at[c, own_slots], 3 + 4 * s + c
        )
        pltpu.make_async_copy(
            fsend.at[c, own_slots], frecv.at[c, own_slots], local_sem.at[3 + c]
        ).start()

    def reflect(s, c):
        v, h = c // 2, c % 2
        lanes = slice(h * width, (h + 1) * width)
        await_bytes(frecv.at[c, others], all_r.at[3 + 4 * s + c])
        pltpu.make_async_copy(
            fsend.at[c, own_slots], frecv.at[c, own_slots], local_sem.at[3 + c]
        ).wait()
        goal = jnp.concatenate([target[m, v, :, lanes] for m in range(modes)], 0)
        value = dot(select[v], frecv[c].reshape(places_n * ray_block, width))
        if s:
            result[:, v, :, lanes] = value.reshape(modes, rays // modes, width)
            await_bytes(bsend.at[c, others], all_s.at[11 + c])
        value = value - goal.astype(F32)
        ray[pl.ds(0, BLK_DEV)] = value.astype(BF).reshape(BLK_DEV, ray_block, width)

        def answer(p, carry):
            for k in range(cap):
                bsend[c, p * cap + k] = ray[label_s[p, 0, v * cap + k]]
            return carry

        lax.fori_loop(0, peers, answer, 0, unroll=4)
        to_bricks(
            lambda peer: bsend.at[c, pl.ds(peer * cap, cap)], brecv[c].at[own_slots], 11 + 4 * s + c
        )
        pltpu.make_async_copy(
            bsend.at[c, own_slots], brecv[c].at[own_slots], local_sem.at[7 + c]
        ).start()

    def adjoint(s, c):
        v, h = c // 2, c % 2
        await_bytes(brecv[c].at[others], all_r.at[11 + 4 * s + c])
        pltpu.make_async_copy(
            bsend.at[c, own_slots], brecv[c].at[own_slots], local_sem.at[7 + c]
        ).wait()

        def unpack(i, carry):
            back[i] = brecv[c][table_s[v, 1, i]]
            return carry

        lax.fori_loop(0, slots, unpack, 0, unroll=8)

        def turn(i, carry):
            piece = back[pl.ds(i * BLK_DEV, BLK_DEV)].reshape(rays, width).astype(F32)
            back_t[:, aligned(i, rays)] = piece.T.astype(BF)
            return carry

        lax.fori_loop(0, entries // rays, turn, 0)
        rows = aligned(h * modes + mode, width)

        def body(j, carry):
            cols = aligned(j, tile)
            change[s, v, rows, cols] = dot(back_t[...], weight[v, :, cols]).astype(BF)
            return carry

        lax.fori_loop(0, voxels // tile, body, 0)
        for k, (skip, peer) in enumerate(((hm, right), (0, right), (0, left), (hm, left))):
            part = change.at[
                s, v, pl.ds(pl.multiple_of((h * modes + mode) * width + skip, hm), hm)
            ]
            to_mode(part, part, as_sem.at[s, c, k], ar_sem.at[s, c, k], peer)

    def gather_relay(s, c):
        v, h = c // 2, c % 2
        for k, (giver, skip, peer) in enumerate(((left, hm, right), (right, 0, left))):
            part = change.at[
                s, v, pl.ds(pl.multiple_of((h * modes + giver) * width + skip, hm), hm)
            ]
            await_bytes(part, ar_sem.at[s, c, 2 * k])
            to_mode(part, part, as_sem.at[s, c, 4 + k], ar_sem.at[s, c, 4 + k], peer)

    def gather_end(s, c):
        for k in (1, 3, 4, 5):
            await_bytes(change.at[s, c // 2, pl.ds(0, hm)], ar_sem.at[s, c, k])

    def renew(c, low_chunk, high_chunk):
        u, h = c // 2, c % 2
        part = pl.ds(h * bins // 2, bins // 2)
        at = u * bins + h * bins // 2
        rows = slice(low_chunk * width, high_chunk * width)

        def body(j, carry):
            cols = aligned(j, tile)
            step = dot(gram[rows, at : at + bins // 2], change[0, u, part, cols]).T
            for d in range(low_chunk, high_chunk):
                i = d - low_chunk
                value = pattern[d, cols, :] - LEARN_RATE * step[:, i * width : (i + 1) * width]
                pattern[d, cols, :] = value
                if c == chunks - 1:
                    qlow[d, cols, :] = value.astype(BF)
            return carry

        lax.fori_loop(0, voxels // tile, body, 0)

    def update(s, u, halves, out=False):
        def body(j, carry):
            cols = aligned(j, tile)
            if len(halves) == 2:
                lhs = jnp.concatenate([half_basis(u, h) for h in range(2)], 1)
                step = dot(lhs, change[s, u, :, cols]).T
            else:
                part = pl.ds(halves[0] * bins // 2, bins // 2)
                step = dot(half_basis(u, halves[0]), change[s, u, part, cols]).T
            coef[cols, :] = coef[cols, :] - LEARN_RATE * step
            if out:
                pltpu.make_async_copy(
                    coef.at[cols], coeffs_out.at[cols], load_sem.at[j]
                ).start()
            return carry

        lax.fori_loop(0, voxels // tile, body, 0)

    partial_patterns(0)
    pl.semaphore_wait(barrier, peers - 1 + modes - 1)

    for k in range(1, modes):
        peer = lax.rem(mode + k, modes)
        to_mode(gpart.at[aligned(peer, share)], grecv.at[k - 1], gs_sem.at[k], gr_sem.at[k], peer)
    to_bricks(lambda peer: label_out.at[peer], label_in.at[brick], 0)
    pltpu.make_async_copy(label_out.at[brick], label_in.at[brick], local_sem.at[0]).start()
    scatter_send(0)
    own_pattern(0)
    partial_patterns(1)
    own_pattern(1)
    share_gram()
    for m in range(modes):
        loads[4 + m].wait()
    mlow[...] = chunk[...].astype(BF)
    scatter_relay(0)
    share_measured(0)
    scatter_send(1)
    build_select()
    loads[2].wait()
    scatter_end(0)
    forward(0, 0)
    scatter_relay(1)
    scatter_send(2)
    measured_end(0)
    reflect(0, 0)
    scatter_end(1)
    forward(0, 1)
    scatter_relay(2)
    share_measured(1)
    scatter_send(3)
    loads[3].wait()
    scatter_end(2)
    forward(0, 2)
    scatter_relay(3)
    adjoint(0, 0)
    reflect(0, 1)
    scatter_end(3)
    forward(0, 3)
    gather_relay(0, 0)
    measured_end(1)
    reflect(0, 2)
    hand_gram()
    adjoint(0, 1)
    reflect(0, 3)
    gather_relay(0, 1)
    adjoint(0, 2)
    gather_end(0, 0)
    await_bytes(gram.at[pl.ds(0, peers // 2 * share)], all_r.at[2])
    renew(0, 0, chunks)
    gather_end(0, 1)
    renew(1, 0, chunks)
    gather_relay(0, 2)
    adjoint(0, 3)
    gather_relay(0, 3)
    gather_end(0, 2)
    renew(2, 0, chunks)
    gather_end(0, 3)
    renew(3, 0, 1)
    forward(1, 0)
    renew(3, 1, chunks)
    forward(1, 1)
    update(0, 0, (0, 1))
    reflect(1, 0)
    forward(1, 2)
    reflect(1, 1)
    forward(1, 3)
    share_result(0)
    update(0, 1, (0,))
    adjoint(1, 0)
    reflect(1, 2)
    gather_relay(1, 0)
    update(0, 1, (1,))
    adjoint(1, 1)
    reflect(1, 3)
    gather_relay(1, 1)
    adjoint(1, 2)
    gather_relay(1, 2)
    adjoint(1, 3)
    gather_end(1, 0)
    gather_end(1, 1)
    update(1, 0, (0, 1))
    gather_relay(1, 3)
    share_result(1)
    writes = []

    def write_residual(v):
        result_end(v)
        collected[:, v] = collected[:, v] - chunk[:, v]
        for m in range(modes):
            write = pltpu.make_async_copy(
                collected.at[m, v],
                residual_out.at[v, :, pl.ds(m * mine, mine)],
                write_sem.at[v, m],
            )
            write.start()
            writes.append(write)

    write_residual(0)
    gather_end(1, 2)
    update(1, 1, (0,))
    gather_end(1, 3)
    update(1, 1, (1,), True)
    write_residual(1)

    for k in range(1, modes):
        await_bytes(grecv.at[0], gs_sem.at[k])
        for v in range(views):
            await_bytes(mlow.at[0, v], ts_sem.at[v, k])
            await_bytes(result.at[0, v], rs_sem.at[v, k])
    for c in range(2 * views):
        for k in range(6):
            await_bytes(qrel.at[0, 0], qs_sem.at[c, k])
            for s in range(2):
                await_bytes(change.at[0, 0, pl.ds(0, hm)], as_sem.at[s, c, k])
        await_bytes(fsend.at[c, others], all_s.at[7 + c])
        await_bytes(bsend.at[c, others], all_s.at[15 + c])
    await_bytes(label_in.at[pl.ds(0, peers - 1)], all_s.at[0])
    await_bytes(gram.at[pl.ds(0, (peers // 2 - 1) * share)], all_s.at[1])
    await_bytes(gram.at[pl.ds(0, peers // 2 * share)], all_s.at[2])
    for write in writes:
        write.wait()

    def drain(j, carry):
        cols = aligned(j, tile)
        pltpu.make_async_copy(coef.at[cols], coeffs_out.at[cols], load_sem.at[j]).wait()
        return carry

    lax.fori_loop(0, voxels // tile, drain, 0)


def shards(coeffs, weights, owners, offsets, basis, measured):
    peers, modes = lax.axis_size("brick"), lax.axis_size("mode")
    views, slots, ray_block, voxels = weights.shape
    cap = max(2, slots // peers + 1)
    here, bins = basis.shape[1:]
    mine = bins // modes
    places_n = peers * cap
    rays = BLK_DEV * ray_block
    share = views * mine // peers

    vmem = pl.BlockSpec(memory_space=pltpu.VMEM)
    anywhere = pl.BlockSpec(memory_space=pl.ANY)
    dma = pltpu.SemaphoreType.DMA
    chunks, width = 2 * views, mine // 2
    block = (places_n, ray_block, width)
    coeffs, residual = pl.pallas_call(
        functools.partial(kernel, peers, modes, cap),
        out_shape=(
            jax.ShapeDtypeStruct(coeffs.shape, F32),
            jax.ShapeDtypeStruct(measured.shape, F32),
        ),
        in_specs=[vmem, vmem] + [anywhere] * 4,
        out_specs=(anywhere, anywhere),
        scratch_shapes=[
            pltpu.VMEM(coeffs.shape, F32),
            pltpu.VMEM(coeffs.shape, BF),
            pltpu.VMEM(basis.shape, BF),
            pltpu.VMEM((views, slots * ray_block, voxels), BF),
            pltpu.VMEM((modes, views, rays // modes, mine), F32),
            pltpu.VMEM((modes, views, rays // modes, mine), BF),
            pltpu.VMEM((views, 3, 2, voxels, width), BF),
            pltpu.VMEM((chunks, 2, voxels // 2, width), BF),
            pltpu.VMEM((chunks, 2, voxels, width), BF),
            pltpu.VMEM((chunks, voxels, width), F32),
            pltpu.VMEM((chunks, voxels, width), BF),
            pltpu.VMEM((slots + 1, ray_block, width), BF),
            pltpu.VMEM((chunks,) + block, BF),
            pltpu.VMEM((chunks,) + block, BF),
            pltpu.VMEM((BLK_DEV + 1, ray_block, width), BF),
            pltpu.VMEM((chunks,) + block, BF),
            pltpu.VMEM(block, BF),
            pltpu.VMEM(block, BF),
            pltpu.VMEM(block, BF),
            pltpu.VMEM(block, BF),
            pltpu.VMEM((slots, ray_block, width), BF),
            pltpu.VMEM((width, slots * ray_block), BF),
            pltpu.VMEM((2, views, bins, voxels), BF),
            pltpu.VMEM((views, rays, places_n * ray_block), BF),
            pltpu.VMEM((views * mine, views * bins), BF),
            pltpu.VMEM((modes * share, views * bins), BF),
            pltpu.VMEM((modes - 1, share, views * bins), BF),
            pltpu.VMEM((peers, 1, 128), jnp.int32),
            pltpu.SMEM((peers, 1, 128), jnp.int32),
            pltpu.VMEM((modes, views, rays // modes, mine), F32),
            pltpu.VMEM((modes, views, rays // modes, mine), F32),
            dma((8,)),
            dma((11,)),
            dma((4,)),
            dma((4,)),
            dma((views, 4)),
            dma((views, 4)),
            dma((chunks, 6)),
            dma((chunks, 6)),
            dma((2, chunks, 6)),
            dma((2, chunks, 6)),
            dma((views, 4)),
            dma((views, 4)),
            dma((19,)),
            dma((19,)),
            dma((views, 4)),
            pltpu.VMEM((views, 8, 128), jnp.int32),
            pltpu.SMEM((views, 8, 128), jnp.int32),
            pltpu.VMEM((peers, 128), jnp.int32),
            pltpu.VMEM((peers, 1, 128), jnp.int32),
            pltpu.VMEM((modes, 128, here), BF),
            pltpu.VMEM((modes, views, rays // modes, mine), BF),
        ],
        compiler_params=pltpu.CompilerParams(
            collective_id=0, has_side_effects=True, vmem_limit_bytes=67043328
        ),
    )(owners.reshape(views, 1, slots), offsets, coeffs, weights.reshape(views, -1, voxels), basis, measured)
    return pl.pallas_call(
        hand_over,
        out_shape=(
            jax.ShapeDtypeStruct(coeffs.shape, F32),
            jax.ShapeDtypeStruct(residual.shape, F32),
        ),
        in_specs=[anywhere, anywhere],
        out_specs=(anywhere, anywhere),
        scratch_shapes=[
            pltpu.VMEM(coeffs.shape, F32),
            pltpu.VMEM(residual.shape, F32),
            dma((9,)),
            dma((9,)),
        ],
        compiler_params=pltpu.CompilerParams(vmem_limit_bytes=67043328),
    )(coeffs, residual)


def solution(mesh):
    return jax.shard_map(
        shards,
        mesh=mesh,
        in_specs=(
            P("brick", "mode"),
            P(None, "brick", None, None),
            P(None, "brick", None),
            P(None, "brick"),
            P(None, "mode", None),
            P(None, ("brick", "mode"), None),
        ),
        out_specs=(P("brick", "mode"), P(None, ("brick", "mode"), None)),
        check_vma=False,
    )
```

```python
import functools
import math

import jax
import jax.numpy as jnp
from jax import lax
from jax.experimental import pallas as pl
from jax.experimental.pallas import tpu as pltpu
from jax.sharding import PartitionSpec as P

BLK_DEV = 8
LEARN_RATE = 0.2
BF = jnp.bfloat16
F32 = jnp.float32
MESH = pl.DeviceIdType.MESH


def dot(a, b):
    return jnp.dot(a, b, preferred_element_type=F32)


def hand_over(coeffs, residual, coeffs_out, residual_out, rows, rays, in_sem, out_sem):
    pieces = in_sem.shape[0] - 1
    part = coeffs.shape[0] // pieces
    moves = [(coeffs, rows, coeffs_out, pl.ds(i * part, part)) for i in range(pieces)]
    moves.append((residual, rays, residual_out, pl.ds(0, residual.shape[0])))
    ins = [
        pltpu.make_async_copy(src.at[at], mid.at[at], in_sem.at[i])
        for i, (src, mid, dst, at) in enumerate(moves)
    ]
    outs = [
        pltpu.make_async_copy(mid.at[at], dst.at[at], out_sem.at[i])
        for i, (src, mid, dst, at) in enumerate(moves)
    ]
    for move in ins:
        move.start()
    for first, second in zip(ins, outs):
        first.wait()
        second.start()
    for move in outs:
        move.wait()


def kernel(
    peers,
    modes,
    cap,
    owners,
    offsets,
    coeffs_hbm,
    weights_hbm,
    basis_hbm,
    measured_hbm,
    coeffs_out,
    residual_out,
    coef,
    low,
    basis,
    weight,
    chunk,
    target,
    qsend,
    qrel,
    qrecv,
    pattern,
    qlow,
    proj,
    fsend,
    frecv,
    ray,
    bsend,
    brecv0,
    brecv1,
    brecv2,
    brecv3,
    back,
    back_t,
    change,
    select,
    gram,
    gpart,
    grecv,
    label_in,
    label_s,
    result,
    collected,
    load_sem,
    local_sem,
    gs_sem,
    gr_sem,
    ts_sem,
    tr_sem,
    qs_sem,
    qr_sem,
    as_sem,
    ar_sem,
    rs_sem,
    rr_sem,
    all_s,
    all_r,
    write_sem,
    table,
    table_s,
    label_flat,
    label_out,
    column,
    mlow,
):
    brecv = (brecv0, brecv1, brecv2, brecv3)
    brick, mode = lax.axis_index("brick"), lax.axis_index("mode")
    right, left, far = [lax.rem(mode + k, modes) for k in (1, modes - 1, 2)]
    views, entries, voxels = weights_hbm.shape
    slots, ray_block = proj.shape[0] - 1, proj.shape[1]
    here, bins = basis.shape[1], basis.shape[2]
    mine = bins // modes
    places_n = peers * cap
    rays = BLK_DEV * ray_block
    tile = min(256, voxels)
    width, chunks = mine // 2, 2 * views
    half, hm = voxels // 2, width // 2
    share = gpart.shape[0] // modes

    def aligned(i, n):
        return pl.ds(pl.multiple_of(i * n, n), n)

    def to_mode(src, dst, s, r, peer):
        copy = pltpu.make_async_remote_copy(
            src_ref=src, dst_ref=dst, send_sem=s, recv_sem=r,
            device_id={"mode": peer}, device_id_type=MESH,
        )
        copy.start()

    def await_bytes(ref, sem):
        pltpu.make_async_copy(ref, ref, sem).wait()

    side = math.isqrt(peers // 2)
    deep = peers // (2 * side)

    def partner(dz, dy, dc):
        z = lax.rem(brick // (2 * side) + dz, deep)
        y = lax.rem(lax.rem(brick // 2, side) + dy, side)
        return (z * side + y) * 2 + lax.rem(lax.rem(brick, 2) + dc, 2)

    def to_bricks(src_of, dst, index):
        def body(k, carry):
            q = lax.rem(k * 13, peers)
            peer = partner(q // (2 * side), lax.rem(q // 2, side), lax.rem(q, 2))
            copy = pltpu.make_async_remote_copy(
                src_ref=src_of(peer), dst_ref=dst, send_sem=all_s.at[index],
                recv_sem=all_r.at[index], device_id={"brick": peer}, device_id_type=MESH,
            )
            copy.start()
            return carry

        lax.fori_loop(1, peers, body, 0)

    loads = [
        pltpu.make_async_copy(basis_hbm, basis, load_sem.at[0]),
        pltpu.make_async_copy(coeffs_hbm, coef, load_sem.at[1]),
        pltpu.make_async_copy(weights_hbm.at[0], weight.at[0], load_sem.at[2]),
        pltpu.make_async_copy(weights_hbm.at[1], weight.at[1], load_sem.at[3]),
    ]
    loads += [
        pltpu.make_async_copy(
            measured_hbm.at[:, :, pl.ds(m * mine, mine)], chunk.at[m], load_sem.at[4 + m]
        )
        for m in range(modes)
    ]
    loads[0].start()
    loads[1].start()
    barrier = pltpu.get_barrier_semaphore()

    def greet(k, carry):
        pl.semaphore_signal(
            barrier, inc=1, device_id={"brick": lax.rem(brick + k, peers)}, device_id_type=MESH
        )
        return carry

    lax.fori_loop(1, peers, greet, 0)
    for k in range(1, modes):
        pl.semaphore_signal(
            barrier, inc=1, device_id={"mode": lax.rem(mode + k, modes)}, device_id_type=MESH
        )
    proj[slots] = jnp.zeros(proj.shape[1:], BF)
    ray[BLK_DEV] = jnp.zeros(ray.shape[1:], BF)

    def grid(rows, cols, dim):
        return lax.broadcasted_iota(jnp.int32, (rows, cols), dim)

    entry, lane = grid(slots, 128, 0), grid(slots, 128, 1)
    flat = jnp.full((peers, 128), BLK_DEV, jnp.int32)
    table[...] = jnp.zeros(table.shape, jnp.int32)
    for v in range(views):
        square = grid(slots, slots, 0) == grid(slots, slots, 1)
        owner = jnp.sum(jnp.where(square, owners[v], 0), 1, keepdims=True)
        owner_row = jnp.sum(jnp.where(entry == lane, owner, 0), 0, keepdims=True)
        earlier = (owner == owner_row) & (lane < entry)
        place = owner * cap + jnp.sum(jnp.where(earlier, 1, 0), 1, keepdims=True)
        place_row = jnp.sum(jnp.where(entry == lane, place + 1, 0), 0, keepdims=True) - 1
        offset = jnp.sum(jnp.where(square, offsets[v : v + 1, :], 0), 1, keepdims=True)
        offset_row = jnp.sum(jnp.where(entry == lane, offset, 0), 0, keepdims=True)
        source = jnp.sum(jnp.where(place == lane, entry - slots, 0), 0, keepdims=True) + slots
        table[v, 0:1, :] = source
        table[v, 1:2, :] = place_row
        for k in range(cap):
            hit = place_row == grid(peers, 128, 0) * cap + k
            label = jnp.sum(jnp.where(hit, offset_row - BLK_DEV, 0), 1, keepdims=True) + BLK_DEV
            flat = jnp.where(grid(peers, 128, 1) == v * cap + k, label, flat)
    label_flat[...] = flat

    def spread_labels(i, carry):
        label_out[i] = label_flat[pl.ds(i, 1), :]
        return carry

    lax.fori_loop(0, peers, spread_labels, 0)
    pltpu.make_async_copy(table, table_s, local_sem.at[0]).start()

    loads[0].wait()
    start = brick * share
    view_here, bin_here = start // mine, lax.rem(start, mine)
    window = bin_here // 128
    picked = []
    for m in range(modes):
        lanes = pl.ds(pl.multiple_of(m * mine + window * 128, 128), 128)
        column[m] = basis[view_here, :, lanes].astype(F32).T.astype(BF)
        rows = pl.ds(pl.multiple_of(lax.rem(bin_here, 128), share), share)
        picked.append(column[m, rows, :])
    picked = jnp.concatenate(picked, 0)
    def half_basis(u, h):
        return jnp.concatenate(
            [basis[u, :, m * mine + h * width : m * mine + (h + 1) * width] for m in range(modes)], 1
        )

    for u in range(views):
        for h in range(2):
            at = u * bins + h * bins // 2
            gpart[:, at : at + bins // 2] = dot(picked, half_basis(u, h)).astype(BF)
    loads[1].wait()
    for load in loads[2:]:
        load.start()
    pltpu.make_async_copy(table, table_s, local_sem.at[0]).wait()

    def round_low(i, carry):
        low[aligned(i, tile), :] = coef[aligned(i, tile), :].astype(BF)
        return carry

    lax.fori_loop(0, voxels // tile, round_low, 0)

    lower, upper = pl.ds(0, half), pl.ds(half, half)

    def partial_patterns(v):
        def body(i, carry):
            rows = aligned(i, tile)
            for slot, m in ((0, far), (1, right), (2, left)):
                value = dot(low[rows, :], basis[v, :, aligned(m, mine)]).astype(BF)
                for h in range(2):
                    qsend[v, slot, h, rows, :] = value[:, h * width : (h + 1) * width]
            return carry

        lax.fori_loop(0, voxels // tile, body, 0)

    def own_pattern(v):
        def body(i, carry):
            rows = aligned(i, tile)
            value = dot(low[rows, :], basis[v, :, aligned(mode, mine)])
            for h in range(2):
                pattern[2 * v + h, rows, :] = value[:, h * width : (h + 1) * width]
            return carry

        lax.fori_loop(0, voxels // tile, body, 0)

    def scatter_send(c):
        v, h = c // 2, c % 2
        for k, (slot, part, dst, peer) in enumerate(
            (
                (0, upper, qrel.at[c, 0], right),
                (0, lower, qrel.at[c, 1], left),
                (1, lower, qrecv.at[c, 0, lower], right),
                (2, upper, qrecv.at[c, 1, upper], left),
            )
        ):
            to_mode(qsend.at[v, slot, h, part], dst, qs_sem.at[c, k], qr_sem.at[c, k], peer)

    def scatter_relay(c):
        v, h = c // 2, c % 2
        for k, (slot, start, part, peer) in enumerate(((1, half, upper, right), (2, 0, lower, left))):
            await_bytes(qrel.at[c, k], qr_sem.at[c, k])

            def body(i, carry, k=k, slot=slot, start=start):
                rows = pl.ds(pl.multiple_of(start + i * (tile // 2), tile // 2), tile // 2)
                given = qrel[c, k, aligned(i, tile // 2), :].astype(F32)
                total = qsend[v, slot, h, rows, :].astype(F32) + given
                qsend[v, slot, h, rows, :] = total.astype(BF)
                return carry

            lax.fori_loop(0, half // (tile // 2), body, 0)
            to_mode(
                qsend.at[v, slot, h, part], qrecv.at[c, k, part],
                qs_sem.at[c, 4 + k], qr_sem.at[c, 4 + k], peer,
            )

    def scatter_end(c):
        for k, part in ((2, lower), (3, upper), (4, upper), (5, lower)):
            await_bytes(qrecv.at[c, 0, part], qr_sem.at[c, k])

        def body(i, carry):
            rows = aligned(i, tile)
            total = pattern[c, rows, :] + qrecv[c, 0, rows, :].astype(F32)
            total = total + qrecv[c, 1, rows, :].astype(F32)
            pattern[c, rows, :] = total
            qlow[c, rows, :] = total.astype(BF)
            return carry

        lax.fori_loop(0, voxels // tile, body, 0)

    def share_gram():
        own = aligned(mode, share)
        for k in range(1, modes):
            await_bytes(grecv.at[k - 1], gr_sem.at[k])
        total = gpart[own, :].astype(F32)
        for k in range(1, modes):
            total = total + grecv[k - 1].astype(F32)
        gram[aligned(brick, share), :] = total.astype(BF)
        rows = gram.at[aligned(brick, share)]

        def body(k, carry):
            q = lax.rem(k * 5, peers // 2)
            peer = partner(q // side, lax.rem(q, side), 0)
            copy = pltpu.make_async_remote_copy(
                src_ref=rows, dst_ref=rows, send_sem=all_s.at[1],
                recv_sem=all_r.at[1], device_id={"brick": peer}, device_id_type=MESH,
            )
            copy.start()
            return carry

        lax.fori_loop(1, peers // 2, body, 0)

    def hand_gram():
        await_bytes(gram.at[pl.ds(0, (peers // 2 - 1) * share)], all_r.at[1])
        core = lax.rem(brick, 2)
        twin = brick + 1 - 2 * core

        def body(k, carry):
            rows = gram.at[aligned(2 * k + core, share)]
            copy = pltpu.make_async_remote_copy(
                src_ref=rows, dst_ref=rows, send_sem=all_s.at[2],
                recv_sem=all_r.at[2], device_id={"brick": twin}, device_id_type=MESH,
            )
            copy.start()
            return carry

        lax.fori_loop(0, peers // 2, body, 0)

    def share_measured(v):
        for k in range(1, modes):
            peer = lax.rem(mode + k, modes)
            to_mode(
                mlow.at[peer, v], target.at[mode, v], ts_sem.at[v, k], tr_sem.at[v, k], peer
            )
        pltpu.make_async_copy(mlow.at[mode, v], target.at[mode, v], local_sem.at[1 + v]).start()

    def measured_end(v):
        for k in range(1, modes):
            await_bytes(target.at[0, v], tr_sem.at[v, k])
        pltpu.make_async_copy(mlow.at[mode, v], target.at[mode, v], local_sem.at[1 + v]).wait()

    def share_result(v):
        for k in range(1, modes):
            peer = lax.rem(mode + k, modes)
            to_mode(
                result.at[peer, v], collected.at[mode, v], rs_sem.at[v, k], rr_sem.at[v, k], peer
            )
        pltpu.make_async_copy(
            result.at[mode, v], collected.at[mode, v], local_sem.at[1 + v]
        ).start()

    def result_end(v):
        for k in range(1, modes):
            await_bytes(collected.at[0, v], rr_sem.at[v, k])
        pltpu.make_async_copy(
            result.at[mode, v], collected.at[mode, v], local_sem.at[1 + v]
        ).wait()

    group = 128 // ray_block

    def build_select():
        await_bytes(label_in.at[pl.ds(0, peers - 1)], all_r.at[0])
        pltpu.make_async_copy(label_out.at[brick], label_in.at[brick], local_sem.at[0]).wait()
        lookup = pltpu.make_async_copy(label_in, label_s, local_sem.at[0])
        lookup.start()
        lookup.wait()

        def build(t, carry):
            row = lax.broadcasted_iota(jnp.int32, (rays, 128), 0)
            lane = lax.broadcasted_iota(jnp.int32, (rays, 128), 1)
            for v in range(views):
                want = jnp.zeros((rays, 128), jnp.int32)
                for g in range(group):
                    entry = t * group + g
                    label = label_s[entry // cap, 0, v * cap + entry % cap]
                    inside = (lane >= g * ray_block) & (lane < (g + 1) * ray_block)
                    want = jnp.where(inside, label * ray_block + lane - g * ray_block, want)
                select[v, :, aligned(t, 128)] = jnp.where(want == row, 1.0, 0.0).astype(BF)
            return carry

        lax.fori_loop(0, places_n // group, build, 0)

    own_slots = pl.ds(brick * cap, cap)
    others = pl.ds(0, places_n - cap)

    def forward(s, c):
        v = c // 2

        def body(i, carry):
            value = dot(weight[v, aligned(i, rays), :], qlow[c]).astype(BF)
            proj[pl.ds(i * BLK_DEV, BLK_DEV)] = value.reshape(BLK_DEV, ray_block, width)
            return carry

        lax.fori_loop(0, entries // rays, body, 0)
        if s:
            await_bytes(fsend.at[c, others], all_s.at[3 + c])

        def pack(i, carry):
            fsend[c, i] = proj[table_s[v, 0, i]]
            return carry

        lax.fori_loop(0, places_n, pack, 0, unroll=8)
        to_bricks(
            lambda peer: fsend.at[c, pl.ds(peer * cap, cap)], frecv.at[c, own_slots], 3 + 4 * s + c
        )
        pltpu.make_async_copy(
            fsend.at[c, own_slots], frecv.at[c, own_slots], local_sem.at[3 + c]
        ).start()

    def reflect(s, c):
        v, h = c // 2, c % 2
        lanes = slice(h * width, (h + 1) * width)
        await_bytes(frecv.at[c, others], all_r.at[3 + 4 * s + c])
        pltpu.make_async_copy(
            fsend.at[c, own_slots], frecv.at[c, own_slots], local_sem.at[3 + c]
        ).wait()
        goal = jnp.concatenate([target[m, v, :, lanes] for m in range(modes)], 0)
        value = dot(select[v], frecv[c].reshape(places_n * ray_block, width))
        if s:
            result[:, v, :, lanes] = value.reshape(modes, rays // modes, width)
            await_bytes(bsend.at[c, others], all_s.at[11 + c])
        value = value - goal.astype(F32)
        ray[pl.ds(0, BLK_DEV)] = value.astype(BF).reshape(BLK_DEV, ray_block, width)

        def answer(p, carry):
            for k in range(cap):
                bsend[c, p * cap + k] = ray[label_s[p, 0, v * cap + k]]
            return carry

        lax.fori_loop(0, peers, answer, 0, unroll=4)
        to_bricks(
            lambda peer: bsend.at[c, pl.ds(peer * cap, cap)], brecv[c].at[own_slots], 11 + 4 * s + c
        )
        pltpu.make_async_copy(
            bsend.at[c, own_slots], brecv[c].at[own_slots], local_sem.at[7 + c]
        ).start()

    def adjoint(s, c):
        v, h = c // 2, c % 2
        await_bytes(brecv[c].at[others], all_r.at[11 + 4 * s + c])
        pltpu.make_async_copy(
            bsend.at[c, own_slots], brecv[c].at[own_slots], local_sem.at[7 + c]
        ).wait()

        def unpack(i, carry):
            back[i] = brecv[c][table_s[v, 1, i]]
            return carry

        lax.fori_loop(0, slots, unpack, 0, unroll=8)

        def turn(i, carry):
            piece = back[pl.ds(i * BLK_DEV, BLK_DEV)].reshape(rays, width).astype(F32)
            back_t[:, aligned(i, rays)] = piece.T.astype(BF)
            return carry

        lax.fori_loop(0, entries // rays, turn, 0)
        rows = aligned(h * modes + mode, width)

        def body(j, carry):
            cols = aligned(j, tile)
            change[s, v, rows, cols] = dot(back_t[...], weight[v, :, cols]).astype(BF)
            return carry

        lax.fori_loop(0, voxels // tile, body, 0)
        for k, (skip, peer) in enumerate(((hm, right), (0, right), (0, left), (hm, left))):
            part = change.at[
                s, v, pl.ds(pl.multiple_of((h * modes + mode) * width + skip, hm), hm)
            ]
            to_mode(part, part, as_sem.at[s, c, k], ar_sem.at[s, c, k], peer)

    def gather_relay(s, c):
        v, h = c // 2, c % 2
        for k, (giver, skip, peer) in enumerate(((left, hm, right), (right, 0, left))):
            part = change.at[
                s, v, pl.ds(pl.multiple_of((h * modes + giver) * width + skip, hm), hm)
            ]
            await_bytes(part, ar_sem.at[s, c, 2 * k])
            to_mode(part, part, as_sem.at[s, c, 4 + k], ar_sem.at[s, c, 4 + k], peer)

    def gather_end(s, c):
        for k in (1, 3, 4, 5):
            await_bytes(change.at[s, c // 2, pl.ds(0, hm)], ar_sem.at[s, c, k])

    def renew(c, low_chunk, high_chunk):
        u, h = c // 2, c % 2
        part = pl.ds(h * bins // 2, bins // 2)
        at = u * bins + h * bins // 2
        rows = slice(low_chunk * width, high_chunk * width)

        def body(j, carry):
            cols = aligned(j, tile)
            step = dot(gram[rows, at : at + bins // 2], change[0, u, part, cols]).T
            for d in range(low_chunk, high_chunk):
                i = d - low_chunk
                value = pattern[d, cols, :] - LEARN_RATE * step[:, i * width : (i + 1) * width]
                pattern[d, cols, :] = value
                if c == chunks - 1:
                    qlow[d, cols, :] = value.astype(BF)
            return carry

        lax.fori_loop(0, voxels // tile, body, 0)

    def update(s, u, halves, out=False):
        def body(j, carry):
            cols = aligned(j, tile)
            if len(halves) == 2:
                lhs = jnp.concatenate([half_basis(u, h) for h in range(2)], 1)
                step = dot(lhs, change[s, u, :, cols]).T
            else:
                part = pl.ds(halves[0] * bins // 2, bins // 2)
                step = dot(half_basis(u, halves[0]), change[s, u, part, cols]).T
            coef[cols, :] = coef[cols, :] - LEARN_RATE * step
            if out:
                pltpu.make_async_copy(
                    coef.at[cols], coeffs_out.at[cols], load_sem.at[j]
                ).start()
            return carry

        lax.fori_loop(0, voxels // tile, body, 0)

    partial_patterns(0)
    pl.semaphore_wait(barrier, peers - 1 + modes - 1)

    for k in range(1, modes):
        peer = lax.rem(mode + k, modes)
        to_mode(gpart.at[aligned(peer, share)], grecv.at[k - 1], gs_sem.at[k], gr_sem.at[k], peer)
    to_bricks(lambda peer: label_out.at[peer], label_in.at[brick], 0)
    pltpu.make_async_copy(label_out.at[brick], label_in.at[brick], local_sem.at[0]).start()
    scatter_send(0)
    own_pattern(0)
    partial_patterns(1)
    own_pattern(1)
    share_gram()
    for m in range(modes):
        loads[4 + m].wait()
    mlow[...] = chunk[...].astype(BF)
    scatter_relay(0)
    share_measured(0)
    scatter_send(1)
    build_select()
    loads[2].wait()
    scatter_end(0)
    forward(0, 0)
    scatter_relay(1)
    scatter_send(2)
    measured_end(0)
    reflect(0, 0)
    scatter_relay(2)
    scatter_send(3)
    scatter_end(1)
    forward(0, 1)
    share_measured(1)
    loads[3].wait()
    scatter_end(2)
    scatter_relay(3)
    forward(0, 2)
    adjoint(0, 0)
    reflect(0, 1)
    scatter_end(3)
    forward(0, 3)
    gather_relay(0, 0)
    measured_end(1)
    reflect(0, 2)
    hand_gram()
    adjoint(0, 1)
    reflect(0, 3)
    gather_relay(0, 1)
    adjoint(0, 2)
    gather_end(0, 0)
    await_bytes(gram.at[pl.ds(0, peers // 2 * share)], all_r.at[2])
    renew(0, 0, chunks)
    gather_end(0, 1)
    renew(1, 0, chunks)
    gather_relay(0, 2)
    adjoint(0, 3)
    gather_relay(0, 3)
    gather_end(0, 2)
    renew(2, 0, chunks)
    gather_end(0, 3)
    renew(3, 0, 1)
    forward(1, 0)
    renew(3, 1, chunks)
    forward(1, 1)
    update(0, 0, (0, 1))
    reflect(1, 0)
    forward(1, 2)
    reflect(1, 1)
    forward(1, 3)
    share_result(0)
    update(0, 1, (0,))
    adjoint(1, 0)
    reflect(1, 2)
    gather_relay(1, 0)
    update(0, 1, (1,))
    adjoint(1, 1)
    reflect(1, 3)
    gather_relay(1, 1)
    adjoint(1, 2)
    gather_relay(1, 2)
    adjoint(1, 3)
    gather_end(1, 0)
    gather_end(1, 1)
    update(1, 0, (0, 1))
    gather_relay(1, 3)
    share_result(1)
    writes = []

    def write_residual(v):
        result_end(v)
        collected[:, v] = collected[:, v] - chunk[:, v]
        for m in range(modes):
            write = pltpu.make_async_copy(
                collected.at[m, v],
                residual_out.at[v, :, pl.ds(m * mine, mine)],
                write_sem.at[v, m],
            )
            write.start()
            writes.append(write)

    write_residual(0)
    gather_end(1, 2)
    update(1, 1, (0,))
    gather_end(1, 3)
    update(1, 1, (1,), True)
    write_residual(1)

    for k in range(1, modes):
        await_bytes(grecv.at[0], gs_sem.at[k])
        for v in range(views):
            await_bytes(mlow.at[0, v], ts_sem.at[v, k])
            await_bytes(result.at[0, v], rs_sem.at[v, k])
    for c in range(2 * views):
        for k in range(6):
            await_bytes(qrel.at[0, 0], qs_sem.at[c, k])
            for s in range(2):
                await_bytes(change.at[0, 0, pl.ds(0, hm)], as_sem.at[s, c, k])
        await_bytes(fsend.at[c, others], all_s.at[7 + c])
        await_bytes(bsend.at[c, others], all_s.at[15 + c])
    await_bytes(label_in.at[pl.ds(0, peers - 1)], all_s.at[0])
    await_bytes(gram.at[pl.ds(0, (peers // 2 - 1) * share)], all_s.at[1])
    await_bytes(gram.at[pl.ds(0, peers // 2 * share)], all_s.at[2])
    for write in writes:
        write.wait()

    def drain(j, carry):
        cols = aligned(j, tile)
        pltpu.make_async_copy(coef.at[cols], coeffs_out.at[cols], load_sem.at[j]).wait()
        return carry

    lax.fori_loop(0, voxels // tile, drain, 0)


def shards(coeffs, weights, owners, offsets, basis, measured):
    peers, modes = lax.axis_size("brick"), lax.axis_size("mode")
    views, slots, ray_block, voxels = weights.shape
    cap = max(2, slots // peers + 1)
    here, bins = basis.shape[1:]
    mine = bins // modes
    places_n = peers * cap
    rays = BLK_DEV * ray_block
    share = views * mine // peers

    vmem = pl.BlockSpec(memory_space=pltpu.VMEM)
    anywhere = pl.BlockSpec(memory_space=pl.ANY)
    dma = pltpu.SemaphoreType.DMA
    chunks, width = 2 * views, mine // 2
    block = (places_n, ray_block, width)
    coeffs, residual = pl.pallas_call(
        functools.partial(kernel, peers, modes, cap),
        out_shape=(
            jax.ShapeDtypeStruct(coeffs.shape, F32),
            jax.ShapeDtypeStruct(measured.shape, F32),
        ),
        in_specs=[vmem, vmem] + [anywhere] * 4,
        out_specs=(anywhere, anywhere),
        scratch_shapes=[
            pltpu.VMEM(coeffs.shape, F32),
            pltpu.VMEM(coeffs.shape, BF),
            pltpu.VMEM(basis.shape, BF),
            pltpu.VMEM((views, slots * ray_block, voxels), BF),
            pltpu.VMEM((modes, views, rays // modes, mine), F32),
            pltpu.VMEM((modes, views, rays // modes, mine), BF),
            pltpu.VMEM((views, 3, 2, voxels, width), BF),
            pltpu.VMEM((chunks, 2, voxels // 2, width), BF),
            pltpu.VMEM((chunks, 2, voxels, width), BF),
            pltpu.VMEM((chunks, voxels, width), F32),
            pltpu.VMEM((chunks, voxels, width), BF),
            pltpu.VMEM((slots + 1, ray_block, width), BF),
            pltpu.VMEM((chunks,) + block, BF),
            pltpu.VMEM((chunks,) + block, BF),
            pltpu.VMEM((BLK_DEV + 1, ray_block, width), BF),
            pltpu.VMEM((chunks,) + block, BF),
            pltpu.VMEM(block, BF),
            pltpu.VMEM(block, BF),
            pltpu.VMEM(block, BF),
            pltpu.VMEM(block, BF),
            pltpu.VMEM((slots, ray_block, width), BF),
            pltpu.VMEM((width, slots * ray_block), BF),
            pltpu.VMEM((2, views, bins, voxels), BF),
            pltpu.VMEM((views, rays, places_n * ray_block), BF),
            pltpu.VMEM((views * mine, views * bins), BF),
            pltpu.VMEM((modes * share, views * bins), BF),
            pltpu.VMEM((modes - 1, share, views * bins), BF),
            pltpu.VMEM((peers, 1, 128), jnp.int32),
            pltpu.SMEM((peers, 1, 128), jnp.int32),
            pltpu.VMEM((modes, views, rays // modes, mine), F32),
            pltpu.VMEM((modes, views, rays // modes, mine), F32),
            dma((8,)),
            dma((11,)),
            dma((4,)),
            dma((4,)),
            dma((views, 4)),
            dma((views, 4)),
            dma((chunks, 6)),
            dma((chunks, 6)),
            dma((2, chunks, 6)),
            dma((2, chunks, 6)),
            dma((views, 4)),
            dma((views, 4)),
            dma((19,)),
            dma((19,)),
            dma((views, 4)),
            pltpu.VMEM((views, 8, 128), jnp.int32),
            pltpu.SMEM((views, 8, 128), jnp.int32),
            pltpu.VMEM((peers, 128), jnp.int32),
            pltpu.VMEM((peers, 1, 128), jnp.int32),
            pltpu.VMEM((modes, 128, here), BF),
            pltpu.VMEM((modes, views, rays // modes, mine), BF),
        ],
        compiler_params=pltpu.CompilerParams(
            collective_id=0, has_side_effects=True, vmem_limit_bytes=67043328
        ),
    )(owners.reshape(views, 1, slots), offsets, coeffs, weights.reshape(views, -1, voxels), basis, measured)
    return pl.pallas_call(
        hand_over,
        out_shape=(
            jax.ShapeDtypeStruct(coeffs.shape, F32),
            jax.ShapeDtypeStruct(residual.shape, F32),
        ),
        in_specs=[anywhere, anywhere],
        out_specs=(anywhere, anywhere),
        scratch_shapes=[
            pltpu.VMEM(coeffs.shape, F32),
            pltpu.VMEM(residual.shape, F32),
            dma((9,)),
            dma((9,)),
        ],
        compiler_params=pltpu.CompilerParams(vmem_limit_bytes=67043328),
    )(coeffs, residual)


def solution(mesh):
    return jax.shard_map(
        shards,
        mesh=mesh,
        in_specs=(
            P("brick", "mode"),
            P(None, "brick", None, None),
            P(None, "brick", None),
            P(None, "brick"),
            P(None, "mode", None),
            P(None, ("brick", "mode"), None),
        ),
        out_specs=(P("brick", "mode"), P(None, ("brick", "mode"), None)),
        check_vma=False,
    )
```
